32 devices in a mesh: batch: 2 (over x), py: 4 (over z), px: 4 (over y, core).
Axes of the slice: x: 2, y: 2, z: 4, core: 2. Of those that a mesh axis runs over, the one named last changes fastest.
Arguments:
- pair_rep: bfloat16 [1024, 512, 128], P(('batch', 'px'), 'py'), parts along dimension 0
- pair_mask: int32 [1024, 512], P(('batch', 'px'), 'py'), parts along dimension 0
- ln_in: bfloat16 [2, 2, 128], replicated
- w_in: bfloat16 [2, 128, 640], replicated
- b_in: bfloat16 [2, 640], replicated
- ln_out: bfloat16 [2, 2, 128], replicated
- w_out: bfloat16 [2, 128, 128], replicated
- b_out: bfloat16 [2, 128], replicated
Outputs:
- output: bfloat16 [1024, 512, 128], P(('batch', 'px'), 'py'), parts along dimension 0
There are 2 independent parts. The reference program is written for one: setup_inputs(seed, part) draws one part's arguments, and reference() takes and returns one part's arrays. A program takes and returns all parts, laid end to end along the dimension named above; an argument that names none is the same for every part.
All inputs are finite; a program needn't handle non-finite values.
Results may differ from the reference program's by a relative error of at most 0.00725319.
Values are sent between devices in bfloat16 or wider.
A program may use at most 1 GiB of HBM per device.

```python
import jax
import jax.numpy as jnp
from jax import lax

RESIDUES = 512
PAIR_DIM = 128
HIDDEN_DIM = 128
ROW_BLOCK = min(RESIDUES, 64)
NUM_BLOCKS = RESIDUES // ROW_BLOCK
CHAN_GROUP = min(HIDDEN_DIM, 16)
NUM_GROUPS = HIDDEN_DIM // CHAN_GROUP
LN_EPS = 1e-5


def setup_inputs(seed: int = 0, part: int = 0) -> dict:
    base_key = jax.random.key(seed)
    part_key = jax.random.fold_in(base_key, part)
    key_pair, key_len = jax.random.split(part_key, 2)
    weight_keys = jax.random.split(jax.random.key(seed + 1), 6)
    in_width = 4 * HIDDEN_DIM + PAIR_DIM
    pair_rep = jax.random.normal(key_pair, (RESIDUES, RESIDUES, PAIR_DIM), jnp.float32).astype(jnp.bfloat16)
    length = RESIDUES - jax.random.randint(key_len, (), 0, RESIDUES // 4 + 1)
    valid = (jnp.arange(RESIDUES) < length).astype(jnp.int32)
    pair_mask = valid[:, None] * valid[None, :]
    ln_base = jnp.array([1.0, 0.0], jnp.float32)[None, :, None]
    ln_in = (ln_base + 0.3 * jax.random.normal(weight_keys[0], (2, 2, PAIR_DIM), jnp.float32)).astype(jnp.bfloat16)
    w_in = (jax.random.normal(weight_keys[1], (2, PAIR_DIM, in_width), jnp.float32) * PAIR_DIM ** -0.5).astype(jnp.bfloat16)
    b_in = (0.5 * jax.random.normal(weight_keys[2], (2, in_width), jnp.float32)).astype(jnp.bfloat16)
    ln_out = (ln_base + 0.3 * jax.random.normal(weight_keys[3], (2, 2, HIDDEN_DIM), jnp.float32)).astype(jnp.bfloat16)
    w_out = (jax.random.normal(weight_keys[4], (2, HIDDEN_DIM, PAIR_DIM), jnp.float32) * HIDDEN_DIM ** -0.5).astype(jnp.bfloat16)
    b_out = (0.5 * jax.random.normal(weight_keys[5], (2, PAIR_DIM), jnp.float32)).astype(jnp.bfloat16)
    return {'pair_rep': pair_rep, 'pair_mask': pair_mask, 'ln_in': ln_in, 'w_in': w_in, 'b_in': b_in, 'ln_out': ln_out, 'w_out': w_out, 'b_out': b_out}


def layer_norm(values, ln_gain, ln_shift, norm_axis):
    average = jnp.mean(values, axis=norm_axis, keepdims=True)
    centered = values - average
    variance = jnp.mean(centered * centered, axis=norm_axis, keepdims=True)
    return centered * lax.rsqrt(variance + LN_EPS) * ln_gain + ln_shift


def norm_pairs(pair_rows, ln_in):
    normed = layer_norm(pair_rows.astype(jnp.float32), ln_in[0].astype(jnp.float32), ln_in[1].astype(jnp.float32), -1)
    return normed.astype(jnp.bfloat16)


def gated_operands(pair_rows, mask_rows, ln_in, w_in, b_in):
    proj_width = 4 * HIDDEN_DIM
    normed = norm_pairs(pair_rows, ln_in)
    projected = jnp.einsum('ijd,de->eij', normed.astype(jnp.float32), w_in[:, :proj_width].astype(jnp.float32))
    projected = projected + b_in[:proj_width].astype(jnp.float32)[:, None, None]
    projected = projected.reshape(4, HIDDEN_DIM, ROW_BLOCK, RESIDUES)
    mask_f32 = mask_rows.astype(jnp.float32)[None]
    left_op = mask_f32 * jax.nn.sigmoid(projected[0]) * projected[1]
    right_op = mask_f32 * jax.nn.sigmoid(projected[2]) * projected[3]
    return left_op.astype(jnp.bfloat16), right_op.astype(jnp.bfloat16)


def tri_update(pair_rep, pair_mask, ln_in, w_in, b_in, ln_out, w_out, b_out, outgoing):
    proj_width = 4 * HIDDEN_DIM
    pair_blocks = pair_rep.reshape(NUM_BLOCKS, ROW_BLOCK, RESIDUES, PAIR_DIM)
    mask_blocks = pair_mask.reshape(NUM_BLOCKS, ROW_BLOCK, RESIDUES)
    left_blocks, right_blocks = lax.map(lambda block_in: gated_operands(block_in[0], block_in[1], ln_in, w_in, b_in), (pair_blocks, mask_blocks))
    left_full = left_blocks.transpose(1, 0, 2, 3).reshape(HIDDEN_DIM, RESIDUES, RESIDUES)
    right_full = right_blocks.transpose(1, 0, 2, 3).reshape(HIDDEN_DIM, RESIDUES, RESIDUES)
    right_groups = right_full.reshape(NUM_GROUPS, CHAN_GROUP, RESIDUES, RESIDUES)
    if outgoing:
        left_sel = left_full.reshape(HIDDEN_DIM, NUM_BLOCKS, ROW_BLOCK, RESIDUES).transpose(1, 0, 2, 3)
        left_sel = left_sel.reshape(NUM_BLOCKS, NUM_GROUPS, CHAN_GROUP, ROW_BLOCK, RESIDUES)
        sum_form = 'cik,cjk->cij'
    else:
        left_sel = left_full.reshape(HIDDEN_DIM, RESIDUES, NUM_BLOCKS, ROW_BLOCK).transpose(2, 0, 1, 3)
        left_sel = left_sel.reshape(NUM_BLOCKS, NUM_GROUPS, CHAN_GROUP, RESIDUES, ROW_BLOCK)
        sum_form = 'cki,ckj->cij'
    gain_out = ln_out[0].astype(jnp.float32)[:, None, None]
    shift_out = ln_out[1].astype(jnp.float32)[:, None, None]

    def group_product(group_pair):
        return jnp.einsum(sum_form, group_pair[0].astype(jnp.float32), group_pair[1].astype(jnp.float32))

    def block_update(block_in):
        pair_rows, left_groups = block_in
        tri_sum = lax.map(group_product, (left_groups, right_groups)).reshape(HIDDEN_DIM, ROW_BLOCK, RESIDUES)
        normed_sum = layer_norm(tri_sum, gain_out, shift_out, 0).astype(jnp.bfloat16)
        update = jnp.einsum('cij,cd->ijd', normed_sum.astype(jnp.float32), w_out.astype(jnp.float32))
        update = update + b_out.astype(jnp.float32)
        normed = norm_pairs(pair_rows, ln_in)
        gate_val = jax.nn.sigmoid(jnp.einsum('ijd,de->ije', normed.astype(jnp.float32), w_in[:, proj_width:].astype(jnp.float32)) + b_in[proj_width:].astype(jnp.float32))
        return (pair_rows.astype(jnp.float32) + gate_val * update).astype(jnp.bfloat16)

    new_blocks = lax.map(block_update, (pair_blocks, left_sel))
    return new_blocks.reshape(RESIDUES, RESIDUES, PAIR_DIM)


def reference(pair_rep, pair_mask, ln_in, w_in, b_in, ln_out, w_out, b_out):
    after_out = tri_update(pair_rep, pair_mask, ln_in[0], w_in[0], b_in[0], ln_out[0], w_out[0], b_out[0], True)
    return tri_update(after_out, pair_mask, ln_in[1], w_in[1], b_in[1], ln_out[1], w_out[1], b_out[1], False)
```

```python
import functools

import jax
import jax.numpy as jnp
from jax import lax
from jax.experimental import pallas as pl
from jax.experimental.pallas import tpu as pltpu
from jax.sharding import PartitionSpec as P

LN_EPS = 1e-5
MESH = pl.DeviceIdType.MESH
F32, BF16 = jnp.float32, jnp.bfloat16
ROWS = 16
TO_RIGHT, TO_LEFT, TO_PARTNER, TO_MIRROR = 0, 1, 2, 3


def norm_major(values, gain, shift):
    average = jnp.mean(values, axis=0, keepdims=True)
    centered = values - average
    variance = jnp.mean(centered * centered, axis=0, keepdims=True)
    return centered * lax.rsqrt(variance + LN_EPS) * gain + shift


def remote(src, dst, send_sem, recv_sem, device):
    return pltpu.make_async_remote_copy(src_ref=src, dst_ref=dst, send_sem=send_sem, recv_sem=recv_sem, device_id=device, device_id_type=MESH)


def landed(ref, sem):
    pltpu.make_async_copy(ref, ref, sem).wait()


def project(rows, mask, w_ref, b_ref, base, stage, dst, at):
    w = w_ref[base:base + 256, :]
    for r in range(0, ROWS, 2):
        pair = jnp.concatenate([rows(r), rows(r + 1)], axis=1)
        prod = jnp.dot(w, pair, preferred_element_type=F32)
        for t in range(2):
            gate = prod[:128, 128 * t:128 * t + 128] + b_ref[base:base + 128, :]
            value = prod[128:, 128 * t:128 * t + 128] + b_ref[base + 128:base + 256, :]
            stage[r + t] = mask[r + t:r + t + 1] * jax.nn.sigmoid(gate) * value
    dst[:, pl.ds(at, ROWS), :] = jnp.transpose(stage[...], (1, 0, 2)).astype(BF16)


def finish_rows(n, x_ref, z_row, zn_row, w_ref, b_ref, wo_ref, bo_ref, lo_ref, stage, emit):
    i0 = pl.multiple_of(n * 8, 8)
    x = x_ref[:, pl.ds(i0, 8), :]
    average = jnp.mean(x, axis=0)
    centered = x - average[None]
    variance = jnp.mean(centered * centered, axis=0)
    scale = lax.rsqrt(variance + LN_EPS)
    stage[...] = jnp.transpose(centered * scale[None], (1, 0, 2))
    for r in range(0, 8, 2):
        pair = [(stage[r + t] * lo_ref[0] + lo_ref[1]).astype(BF16) for t in range(2)]
        update = jnp.dot(wo_ref[...], jnp.concatenate(pair, axis=1), preferred_element_type=F32)
        zn = jnp.concatenate([zn_row(i0 + r), zn_row(i0 + r + 1)], axis=1)
        gate = jnp.dot(w_ref[512:640, :], zn, preferred_element_type=F32)
        for t in range(2):
            lanes = slice(128 * t, 128 * t + 128)
            g = jax.nn.sigmoid(gate[:, lanes] + b_ref[512:640, :])
            emit(i0 + r + t, z_row(i0 + r + t).astype(F32) + g * (update[:, lanes] + bo_ref[...]))


def near_order(q, s):
    first = q + 1 - 2 * lax.rem(q, 2)
    second = 2 - lax.div(q, 2)
    third = 3 - 3 * lax.div(q, 2)
    is0, is1, is2, is3 = (jnp.int32(1) * (s == v) for v in range(4))
    return is0 * q + is1 * first + is2 * second + is3 * third


def greet(p, q, everyone):
    barrier = pltpu.get_barrier_semaphore()
    peers = [lax.rem(p + d, 4) for d in (1, 2, 3)] if everyone else [p + 1 - 2 * lax.rem(p, 2), lax.rem(p + 2, 4)]
    for peer in peers:
        pl.semaphore_signal(barrier, inc=1, device_id={'px': peer}, device_id_type=MESH)

    @pl.when(q < 3)
    def _():
        pl.semaphore_signal(barrier, inc=1, device_id={'py': q + 1}, device_id_type=MESH)

    @pl.when(q > 0)
    def _():
        pl.semaphore_signal(barrier, inc=1, device_id={'py': q - 1}, device_id_type=MESH)

    edge = jnp.int32(1) * (q == 0) + jnp.int32(1) * (q == 3)
    pl.semaphore_wait(barrier, len(peers) + 2 - edge)


def outgoing_kernel(z_ref, mask_ref, w_ref, b_ref, li_ref, wo_ref, bo_ref, lo_ref, out_ref,
                    zb, mb, a_ref, bb_ref, x_ref, stage, stage8, ra, rb, rma, rmb, ss, sm):
    chunks = 128 // ROWS
    p, q = lax.axis_index('px'), lax.axis_index('py')
    partner, mirror = p + 1 - 2 * lax.rem(p, 2), lax.rem(p + 2, 4)
    right, left = {'py': q + 1}, {'py': q - 1}
    diag = p == q
    relay = p == lax.rem(q + 2, 4)
    bsel = 1 - jnp.int32(1) * diag

    greet(p, q, False)

    def rows_of(h):
        return pl.ds(pl.multiple_of(h * ROWS, ROWS), ROWS)

    def along(k, h, kind, dev):
        part = zb.at[0, k, rows_of(h)]
        remote(part, part, ss.at[kind, k], ra.at[k, h], dev).start()

    def across(which, k, h, kind, dev):
        remote(zb.at[which, k, rows_of(h)], zb.at[1, k, rows_of(h)], ss.at[kind, k], rb.at[k, h], dev).start()

    def along_mask(k, kind, dev):
        remote(mb.at[0, k], mb.at[0, k], sm.at[kind, k], rma.at[k], dev).start()

    def across_mask(which, k, kind, dev):
        remote(mb.at[which, k], mb.at[1, k], sm.at[kind, k], rmb.at[k], dev).start()

    def spread(k, h, first):
        @pl.when(jnp.logical_and(q < 3, k <= q))
        def _():
            along(k, h, TO_RIGHT, right)
            if first is not None:
                pl.when(first)(lambda: along_mask(k, TO_RIGHT, right))

        @pl.when(jnp.logical_and(q > 0, k >= q))
        def _():
            along(k, h, TO_LEFT, left)
            if first is not None:
                pl.when(first)(lambda: along_mask(k, TO_LEFT, left))

        @pl.when(diag)
        def _():
            across(0, k, h, TO_MIRROR, {'px': mirror})
            across(0, k, h, TO_PARTNER, {'px': partner})
            if first is not None:
                @pl.when(first)
                def _():
                    across_mask(0, k, TO_MIRROR, {'px': mirror})
                    across_mask(0, k, TO_PARTNER, {'px': partner})

    mb[0, q] = mask_ref[...]

    @pl.loop(0, chunks)
    def _(h):
        for r in range(ROWS):
            i = h * ROWS + r
            zt = jnp.transpose(z_ref[i].astype(F32))
            out_ref[i] = zt.astype(BF16)
            zb[0, q, i] = norm_major(zt, li_ref[0], li_ref[1]).astype(BF16)

        @pl.when(h > 0)
        def _():
            spread(q, h - 1, h == 1)

    @pl.loop(0, 128)
    def _(c):
        x_ref[c] = jnp.zeros((128, 128), F32)

    spread(q, jnp.int32(chunks - 1), None)

    @pl.loop(0, 4)
    def _(s):
        k = near_order(q, s)

        @pl.loop(0, chunks)
        def _(h):
            @pl.when(s > 0)
            def _():
                landed(zb.at[0, k, rows_of(h)], ra.at[k, h])
                pl.when(h == 0)(lambda: landed(mb.at[0, k], rma.at[k]))
                spread(k, h, h == 0)

            @pl.when(jnp.logical_not(diag))
            def _():
                landed(zb.at[1, k, rows_of(h)], rb.at[k, h])
                pl.when(h == 0)(lambda: landed(mb.at[1, k], rmb.at[k]))

                @pl.when(relay)
                def _():
                    across(1, k, h, TO_PARTNER, {'px': partner})
                    pl.when(h == 0)(lambda: across_mask(1, k, TO_PARTNER, {'px': partner}))

            r0 = pl.multiple_of(h * ROWS, ROWS)
            mask_a = mb[0, k, pl.ds(r0, ROWS), :].astype(F32)
            project(lambda r: zb[0, k, r0 + r], mask_a, w_ref, b_ref, 0, stage, a_ref, r0)
            mask_b = mb[bsel, k, pl.ds(r0, ROWS), :].astype(F32)
            project(lambda r: zb[bsel, k, r0 + r], mask_b, w_ref, b_ref, 256, stage, bb_ref, r0)

        @pl.loop(0, 128 // 16)
        def _(n):
            for u in range(16):
                c = n * 16 + u
                x_ref[c] += lax.dot_general(a_ref[c], bb_ref[c], (((1,), (1,)), ((), ())), preferred_element_type=F32)

    @pl.loop(0, 16)
    def _(n):
        def emit(i, value):
            out_ref[i] = value.astype(BF16)
        finish_rows(n, x_ref, lambda i: out_ref[i], lambda i: zb[0, q, i], w_ref, b_ref, wo_ref, bo_ref, lo_ref, stage8, emit)

    for k in range(4):
        def drain(kind, when):
            @pl.when(when)
            def _():
                landed(zb.at[0, k], ss.at[kind, k])
                landed(mb.at[0, k], sm.at[kind, k])
        drain(TO_RIGHT, jnp.logical_and(q < 3, k <= q))
        drain(TO_LEFT, jnp.logical_and(q > 0, k >= q))
        drain(TO_MIRROR, diag)
        drain(TO_PARTNER, jnp.logical_or(diag, relay))


VM = pl.BlockSpec(memory_space=pltpu.VMEM)
ANY = pl.BlockSpec(memory_space=pl.ANY)
DMA = pltpu.SemaphoreType.DMA


def outgoing(z, mask, wt, bias, ln_in, wo, bo, ln_out):
    return pl.pallas_call(
        outgoing_kernel,
        out_shape=jax.ShapeDtypeStruct((128, 128, 128), BF16),
        in_specs=[VM] * 8,
        out_specs=VM,
        scratch_shapes=[
            pltpu.VMEM((2, 4, 128, 128, 128), BF16),
            pltpu.VMEM((2, 4, 128, 128), BF16),
            pltpu.VMEM((128, 128, 128), BF16),
            pltpu.VMEM((128, 128, 128), BF16),
            pltpu.VMEM((128, 128, 128), F32),
            pltpu.VMEM((ROWS, 128, 128), F32),
            pltpu.VMEM((8, 128, 128), F32),
            DMA((4, 128 // ROWS)), DMA((4, 128 // ROWS)), DMA((4,)), DMA((4,)), DMA((4, 4)), DMA((4, 4)),
        ],
        compiler_params=pltpu.CompilerParams(collective_id=0, has_side_effects=True, vmem_limit_bytes=67043328),
        name='outgoing',
    )(z, mask, wt, bias, ln_in, wo, bo, ln_out)


def incoming_kernel(z_ref, mask_ref, w_ref, b_ref, li_ref, wo_ref, bo_ref, lo_ref, out_ref, col,
                    zz, mm, mc, a_ref, bb_ref, x_ref, stage, stage8, rc, ra, rb, lc, rmc, rma, rmb, io, ss, sm, sp, spm):
    chunks = 128 // ROWS
    p, q = lax.axis_index('px'), lax.axis_index('py')
    partner, mirror = p + 1 - 2 * lax.rem(p, 2), lax.rem(p + 2, 4)
    right, left = {'py': q + 1}, {'py': q - 1}
    diag = p == q
    off_diag = jnp.logical_not(diag)
    asel = jnp.int32(1) * diag

    greet(p, q, True)
    load = pltpu.make_async_copy(z_ref, a_ref.at[:, 0:128, :], io.at[0])
    load.start()

    def rows_of(h):
        return pl.ds(pl.multiple_of(h * ROWS, ROWS), ROWS)

    def to_line(src, m, h, kind, dev):
        remote(src, col.at[m, rows_of(h)], ss.at[kind, m], rc.at[m, h], dev).start()

    def to_line_mask(src, m, kind, dev):
        remote(src, mc.at[m], sm.at[kind, m], rmc.at[m], dev).start()

    def plane(src, which, k, h, sem, rsem, dev):
        remote(src, zz.at[which, k, rows_of(h)], sem, rsem, dev).start()

    def own(h, first):
        part = zz.at[1, p, rows_of(h)]

        @pl.when(q < 3)
        def _():
            to_line(part, q, h, TO_RIGHT, right)
            if first is not None:
                pl.when(first)(lambda: to_line_mask(mm.at[1, p], q, TO_RIGHT, right))

        @pl.when(q > 0)
        def _():
            to_line(part, q, h, TO_LEFT, left)
            if first is not None:
                pl.when(first)(lambda: to_line_mask(mm.at[1, p], q, TO_LEFT, left))
        plane(part, 1, p, h, sp.at[0], rb.at[p, h], {'px': mirror})
        plane(part, 1, p, h, sp.at[1], rb.at[p, h], {'px': partner})
        if first is not None:
            @pl.when(first)
            def _():
                remote(mm.at[1, p], mm.at[1, p], spm.at[0], rmb.at[p], {'px': mirror}).start()
                remote(mm.at[1, p], mm.at[1, p], spm.at[1], rmb.at[p], {'px': partner}).start()

    mm[1, p] = mask_ref[...]
    load.wait()

    @pl.loop(0, chunks)
    def _(h):
        for r in range(ROWS):
            i = h * ROWS + r
            zt = a_ref[i, 0:128, :].astype(F32)
            zz[1, p, i] = norm_major(zt, li_ref[0], li_ref[1]).astype(BF16)

        @pl.when(h > 0)
        def _():
            own(h - 1, h == 1)

    @pl.loop(0, 128)
    def _(c):
        x_ref[c] = jnp.zeros((128, 128), F32)

    own(jnp.int32(chunks - 1), None)

    def pass_on(s, m, h):
        landed(col.at[m, rows_of(h)], rc.at[m, h])
        pl.when(h == 0)(lambda: landed(mc.at[m], rmc.at[m]))
        part = col.at[m, rows_of(h)]

        @pl.when(jnp.logical_and(q < 3, m < q))
        def _():
            to_line(part, m, h, TO_RIGHT, right)
            pl.when(h == 0)(lambda: to_line_mask(mc.at[m], m, TO_RIGHT, right))

        @pl.when(jnp.logical_and(q > 0, m > q))
        def _():
            to_line(part, m, h, TO_LEFT, left)
            pl.when(h == 0)(lambda: to_line_mask(mc.at[m], m, TO_LEFT, left))

        @pl.when(m != p)
        def _():
            plane(part, 0, p, h, ss.at[2, m], ra.at[p, h], {'px': m})
            pl.when(h == 0)(lambda: remote(mc.at[m], mm.at[0, p], sm.at[2, m], rma.at[p], {'px': m}).start())

        @pl.when(m == p)
        def _():
            pltpu.make_async_copy(part, zz.at[0, p, rows_of(h)], lc.at[h]).start()

            @pl.when(h == 0)
            def _():
                mm[0, p] = mc[p]

        @pl.when(s == 1)
        def _():
            landed(zz.at[1, mirror, rows_of(h)], rb.at[mirror, h])
            plane(zz.at[1, mirror, rows_of(h)], 1, mirror, h, sp.at[2], rb.at[mirror, h], {'px': partner})

            @pl.when(h == 0)
            def _():
                landed(mm.at[1, mirror], rmb.at[mirror])
                remote(mm.at[1, mirror], mm.at[1, mirror], spm.at[2], rmb.at[mirror], {'px': partner}).start()

    def compute(h):
        r0 = pl.multiple_of(h * ROWS, ROWS)

        @pl.loop(0, 4)
        def _(k):
            @pl.when(jnp.logical_and(k != p, k != mirror))
            def _():
                landed(zz.at[1, k, rows_of(h)], rb.at[k, h])
                pl.when(h == 0)(lambda: landed(mm.at[1, k], rmb.at[k]))

            @pl.when(jnp.logical_and(off_diag, k != p))
            def _():
                landed(zz.at[0, k, rows_of(h)], ra.at[k, h])
                pl.when(h == 0)(lambda: landed(mm.at[0, k], rma.at[k]))

            @pl.when(jnp.logical_and(off_diag, k == p))
            def _():
                landed(zz.at[0, k, rows_of(h)], lc.at[h])

            at = pl.multiple_of(k * 64 + lax.rem(h, 4) * ROWS, ROWS)
            mask_b = mm[1, k, pl.ds(r0, ROWS), :].astype(F32)
            project(lambda r: zz[1, k, r0 + r], mask_b, w_ref, b_ref, 256, stage, bb_ref, at)
            mask_a = mm[asel, k, pl.ds(r0, ROWS), :].astype(F32)
            project(lambda r: zz[asel, k, r0 + r], mask_a, w_ref, b_ref, 0, stage, a_ref, at)

        @pl.when(lax.rem(h, 4) == 3)
        def _():
            @pl.loop(0, 128 // 8)
            def _(n):
                for u in range(8):
                    c = n * 8 + u
                    x_ref[c] += lax.dot_general(a_ref[c], bb_ref[c], (((0,), (0,)), ((), ())), preferred_element_type=F32)

    @pl.loop(1, 4)
    def _(s):
        m = near_order(q, s)
        mine = jnp.logical_or(m == p, jnp.logical_and(diag, s == 1))

        @pl.loop(0, chunks + 1)
        def _(h):
            @pl.when(h < chunks)
            def _():
                pass_on(s, m, h)

            @pl.when(jnp.logical_and(h > 0, mine))
            def _():
                compute(h - 1)

    load.start()
    load.wait()

    def store(n):
        rows = pl.ds(pl.multiple_of(n * 8, 8), 8)
        return pltpu.make_async_copy(bb_ref.at[rows, 0:128, :], out_ref.at[rows], io.at[1])

    @pl.loop(0, 16)
    def _(n):
        def emit(i, value):
            bb_ref[i, 0:128, :] = jnp.transpose(value).astype(BF16)
        finish_rows(n, x_ref, lambda i: a_ref[i, 0:128, :], lambda i: zz[1, p, i], w_ref, b_ref, wo_ref, bo_ref, lo_ref, stage8, emit)
        pl.when(n > 0)(lambda: store(n - 1).start())

    store(jnp.int32(15)).start()

    for m in range(4):
        def drain(kind, when):
            @pl.when(when)
            def _():
                landed(col.at[m], ss.at[kind, m])
                landed(mc.at[m], sm.at[kind, m])
        drain(TO_RIGHT, jnp.logical_and(q < 3, m <= q))
        drain(TO_LEFT, jnp.logical_and(q > 0, m >= q))
        drain(2, jnp.logical_and(m != q, m != p))
    for kind in range(3):
        landed(zz.at[1, 0], sp.at[kind])
        landed(mm.at[1, 0], spm.at[kind])
    pltpu.make_async_copy(bb_ref.at[:, 0:128, :], out_ref, io.at[1]).wait()


def incoming(z, mask, wt, bias, ln_in, wo, bo, ln_out):
    n = 128 // ROWS
    return pl.pallas_call(
        incoming_kernel,
        out_shape=[jax.ShapeDtypeStruct((128, 128, 128), BF16), jax.ShapeDtypeStruct((4, 128, 128, 128), BF16)],
        in_specs=[ANY] + [VM] * 7,
        out_specs=[ANY, ANY],
        scratch_shapes=[
            pltpu.VMEM((2, 4, 128, 128, 128), BF16),
            pltpu.VMEM((2, 4, 128, 128), BF16),
            pltpu.VMEM((4, 128, 128), BF16),
            pltpu.VMEM((128, 256, 128), BF16),
            pltpu.VMEM((128, 256, 128), BF16),
            pltpu.VMEM((128, 128, 128), F32),
            pltpu.VMEM((ROWS, 128, 128), F32),
            pltpu.VMEM((8, 128, 128), F32),
            DMA((4, n)), DMA((4, n)), DMA((4, n)), DMA((n,)), DMA((4,)), DMA((4,)), DMA((4,)), DMA((2,)),
            DMA((3, 4)), DMA((3, 4)), DMA((3,)), DMA((3,)),
        ],
        compiler_params=pltpu.CompilerParams(collective_id=1, has_side_effects=True, vmem_limit_bytes=67043328),
        name='incoming',
    )(z, mask, wt, bias, ln_in, wo, bo, ln_out)[0]


def solution(mesh):
    pair_spec = P(('batch', 'px'), 'py', None)
    mask_spec = P(('batch', 'px'), 'py')
    whole = P()

    def device_body(pair_blk, mask_blk, ln_in, w_in, b_in, ln_out, w_out, b_out):
        mask = mask_blk.astype(BF16)
        wt = jnp.swapaxes(w_in, 1, 2)
        wo = jnp.swapaxes(w_out, 1, 2)
        def wide(v):
            return jnp.broadcast_to(v.astype(F32)[..., None], v.shape + (128,))
        bias, bo, li, lo = wide(b_in), wide(b_out), wide(ln_in), wide(ln_out)
        z1 = outgoing(pair_blk, mask, wt[0], bias[0], li[0], wo[0], bo[0], lo[0])
        return incoming(z1, mask, wt[1], bias[1], li[1], wo[1], bo[1], lo[1])

    return jax.shard_map(device_body, mesh=mesh, in_specs=(pair_spec, mask_spec, whole, whole, whole, whole, whole, whole), out_specs=pair_spec, check_vma=False)
```

```python
import functools

import jax
import jax.numpy as jnp
from jax import lax
from jax.experimental import pallas as pl
from jax.experimental.pallas import tpu as pltpu
from jax.sharding import PartitionSpec as P

LN_EPS = 1e-5
MESH = pl.DeviceIdType.MESH
F32, BF16 = jnp.float32, jnp.bfloat16
ROWS = 16
TO_RIGHT, TO_LEFT, TO_PARTNER, TO_MIRROR = 0, 1, 2, 3


def norm_major(values, gain, shift):
    average = jnp.mean(values, axis=0, keepdims=True)
    centered = values - average
    variance = jnp.mean(centered * centered, axis=0, keepdims=True)
    return centered * lax.rsqrt(variance + LN_EPS) * gain + shift


def remote(src, dst, send_sem, recv_sem, device):
    return pltpu.make_async_remote_copy(src_ref=src, dst_ref=dst, send_sem=send_sem, recv_sem=recv_sem, device_id=device, device_id_type=MESH)


def landed(ref, sem):
    pltpu.make_async_copy(ref, ref, sem).wait()


def project(rows, mask, w_ref, b_ref, base, stage, dst, at):
    w = w_ref[base:base + 256, :]
    for r in range(0, ROWS, 2):
        pair = jnp.concatenate([rows(r), rows(r + 1)], axis=1)
        prod = jnp.dot(w, pair, preferred_element_type=F32)
        for t in range(2):
            gate = prod[:128, 128 * t:128 * t + 128] + b_ref[base:base + 128, :]
            value = prod[128:, 128 * t:128 * t + 128] + b_ref[base + 128:base + 256, :]
            stage[r + t] = mask[r + t:r + t + 1] * jax.nn.sigmoid(gate) * value
    dst[:, pl.ds(at, ROWS), :] = jnp.transpose(stage[...], (1, 0, 2)).astype(BF16)


def finish_rows(n, x_ref, z_row, zn_row, w_ref, b_ref, wo_ref, bo_ref, lo_ref, stage, emit):
    i0 = pl.multiple_of(n * 8, 8)
    x = x_ref[:, pl.ds(i0, 8), :]
    average = jnp.mean(x, axis=0)
    centered = x - average[None]
    variance = jnp.mean(centered * centered, axis=0)
    scale = lax.rsqrt(variance + LN_EPS)
    stage[...] = jnp.transpose(centered * scale[None], (1, 0, 2))
    for r in range(0, 8, 2):
        pair = [(stage[r + t] * lo_ref[0] + lo_ref[1]).astype(BF16) for t in range(2)]
        update = jnp.dot(wo_ref[...], jnp.concatenate(pair, axis=1), preferred_element_type=F32)
        zn = jnp.concatenate([zn_row(i0 + r), zn_row(i0 + r + 1)], axis=1)
        gate = jnp.dot(w_ref[512:640, :], zn, preferred_element_type=F32)
        for t in range(2):
            lanes = slice(128 * t, 128 * t + 128)
            g = jax.nn.sigmoid(gate[:, lanes] + b_ref[512:640, :])
            emit(i0 + r + t, z_row(i0 + r + t).astype(F32) + g * (update[:, lanes] + bo_ref[...]))


def near_order(q, s):
    first = q + 1 - 2 * lax.rem(q, 2)
    second = 2 - lax.div(q, 2)
    third = 3 - 3 * lax.div(q, 2)
    is0, is1, is2, is3 = (jnp.int32(1) * (s == v) for v in range(4))
    return is0 * q + is1 * first + is2 * second + is3 * third


def greet(p, q, everyone):
    barrier = pltpu.get_barrier_semaphore()
    peers = [lax.rem(p + d, 4) for d in (1, 2, 3)] if everyone else [p + 1 - 2 * lax.rem(p, 2), lax.rem(p + 2, 4)]
    for peer in peers:
        pl.semaphore_signal(barrier, inc=1, device_id={'px': peer}, device_id_type=MESH)

    @pl.when(q < 3)
    def _():
        pl.semaphore_signal(barrier, inc=1, device_id={'py': q + 1}, device_id_type=MESH)

    @pl.when(q > 0)
    def _():
        pl.semaphore_signal(barrier, inc=1, device_id={'py': q - 1}, device_id_type=MESH)

    edge = jnp.int32(1) * (q == 0) + jnp.int32(1) * (q == 3)
    pl.semaphore_wait(barrier, len(peers) + 2 - edge)


def outgoing_kernel(z_ref, mask_ref, w_ref, b_ref, li_ref, wo_ref, bo_ref, lo_ref, out_ref,
                    zb, mb, a_ref, bb_ref, x_ref, stage, stage8, ra, rb, rma, rmb, ss, sm):
    chunks = 128 // ROWS
    p, q = lax.axis_index('px'), lax.axis_index('py')
    partner, mirror = p + 1 - 2 * lax.rem(p, 2), lax.rem(p + 2, 4)
    right, left = {'py': q + 1}, {'py': q - 1}
    diag = p == q
    relay = p == lax.rem(q + 2, 4)
    bsel = 1 - jnp.int32(1) * diag

    greet(p, q, False)

    def rows_of(h):
        return pl.ds(pl.multiple_of(h * ROWS, ROWS), ROWS)

    def along(k, h, kind, dev):
        part = zb.at[0, k, rows_of(h)]
        remote(part, part, ss.at[kind, k], ra.at[k, h], dev).start()

    def across(which, k, h, kind, dev):
        remote(zb.at[which, k, rows_of(h)], zb.at[1, k, rows_of(h)], ss.at[kind, k], rb.at[k, h], dev).start()

    def along_mask(k, kind, dev):
        remote(mb.at[0, k], mb.at[0, k], sm.at[kind, k], rma.at[k], dev).start()

    def across_mask(which, k, kind, dev):
        remote(mb.at[which, k], mb.at[1, k], sm.at[kind, k], rmb.at[k], dev).start()

    def spread(k, h, first):
        @pl.when(jnp.logical_and(q < 3, k <= q))
        def _():
            along(k, h, TO_RIGHT, right)
            if first is not None:
                pl.when(first)(lambda: along_mask(k, TO_RIGHT, right))

        @pl.when(jnp.logical_and(q > 0, k >= q))
        def _():
            along(k, h, TO_LEFT, left)
            if first is not None:
                pl.when(first)(lambda: along_mask(k, TO_LEFT, left))

        @pl.when(diag)
        def _():
            across(0, k, h, TO_MIRROR, {'px': mirror})
            across(0, k, h, TO_PARTNER, {'px': partner})
            if first is not None:
                @pl.when(first)
                def _():
                    across_mask(0, k, TO_MIRROR, {'px': mirror})
                    across_mask(0, k, TO_PARTNER, {'px': partner})

    mb[0, q] = mask_ref[...]

    @pl.loop(0, chunks)
    def _(h):
        for r in range(ROWS):
            i = h * ROWS + r
            zt = jnp.transpose(z_ref[i].astype(F32))
            out_ref[i] = zt.astype(BF16)
            zb[0, q, i] = norm_major(zt, li_ref[0], li_ref[1]).astype(BF16)

        @pl.when(h > 0)
        def _():
            spread(q, h - 1, h == 1)

    @pl.loop(0, 128)
    def _(c):
        x_ref[c] = jnp.zeros((128, 128), F32)

    spread(q, jnp.int32(chunks - 1), None)

    @pl.loop(0, 4)
    def _(s):
        k = near_order(q, s)

        @pl.loop(0, chunks)
        def _(h):
            @pl.when(s > 0)
            def _():
                landed(zb.at[0, k, rows_of(h)], ra.at[k, h])
                pl.when(h == 0)(lambda: landed(mb.at[0, k], rma.at[k]))
                spread(k, h, h == 0)

            @pl.when(jnp.logical_not(diag))
            def _():
                landed(zb.at[1, k, rows_of(h)], rb.at[k, h])
                pl.when(h == 0)(lambda: landed(mb.at[1, k], rmb.at[k]))

                @pl.when(relay)
                def _():
                    across(1, k, h, TO_PARTNER, {'px': partner})
                    pl.when(h == 0)(lambda: across_mask(1, k, TO_PARTNER, {'px': partner}))

            r0 = pl.multiple_of(h * ROWS, ROWS)
            mask_a = mb[0, k, pl.ds(r0, ROWS), :].astype(F32)
            project(lambda r: zb[0, k, r0 + r], mask_a, w_ref, b_ref, 0, stage, a_ref, r0)
            mask_b = mb[bsel, k, pl.ds(r0, ROWS), :].astype(F32)
            project(lambda r: zb[bsel, k, r0 + r], mask_b, w_ref, b_ref, 256, stage, bb_ref, r0)

        @pl.loop(0, 128 // 16)
        def _(n):
            for u in range(16):
                c = n * 16 + u
                x_ref[c] += lax.dot_general(a_ref[c], bb_ref[c], (((1,), (1,)), ((), ())), preferred_element_type=F32)

    @pl.loop(0, 16)
    def _(n):
        def emit(i, value):
            out_ref[i] = value.astype(BF16)
        finish_rows(n, x_ref, lambda i: out_ref[i], lambda i: zb[0, q, i], w_ref, b_ref, wo_ref, bo_ref, lo_ref, stage8, emit)

    for k in range(4):
        def drain(kind, when):
            @pl.when(when)
            def _():
                landed(zb.at[0, k], ss.at[kind, k])
                landed(mb.at[0, k], sm.at[kind, k])
        drain(TO_RIGHT, jnp.logical_and(q < 3, k <= q))
        drain(TO_LEFT, jnp.logical_and(q > 0, k >= q))
        drain(TO_MIRROR, diag)
        drain(TO_PARTNER, jnp.logical_or(diag, relay))


VM = pl.BlockSpec(memory_space=pltpu.VMEM)
ANY = pl.BlockSpec(memory_space=pl.ANY)
DMA = pltpu.SemaphoreType.DMA


def outgoing(z, mask, wt, bias, ln_in, wo, bo, ln_out):
    return pl.pallas_call(
        outgoing_kernel,
        out_shape=jax.ShapeDtypeStruct((128, 128, 128), BF16),
        in_specs=[VM] * 8,
        out_specs=VM,
        scratch_shapes=[
            pltpu.VMEM((2, 4, 128, 128, 128), BF16),
            pltpu.VMEM((2, 4, 128, 128), BF16),
            pltpu.VMEM((128, 128, 128), BF16),
            pltpu.VMEM((128, 128, 128), BF16),
            pltpu.VMEM((128, 128, 128), F32),
            pltpu.VMEM((ROWS, 128, 128), F32),
            pltpu.VMEM((8, 128, 128), F32),
            DMA((4, 128 // ROWS)), DMA((4, 128 // ROWS)), DMA((4,)), DMA((4,)), DMA((4, 4)), DMA((4, 4)),
        ],
        compiler_params=pltpu.CompilerParams(collective_id=0, has_side_effects=True, vmem_limit_bytes=67043328),
        name='outgoing',
    )(z, mask, wt, bias, ln_in, wo, bo, ln_out)


def incoming_kernel(z_ref, mask_ref, w_ref, b_ref, li_ref, wo_ref, bo_ref, lo_ref, out_ref, col,
                    zz, mm, mc, a_ref, bb_ref, x_ref, stage, stage8, rc, ra, rb, lc, rmc, rma, rmb, io, ss, sm, sp, spm):
    chunks = 128 // ROWS
    p, q = lax.axis_index('px'), lax.axis_index('py')
    partner, mirror = p + 1 - 2 * lax.rem(p, 2), lax.rem(p + 2, 4)
    right, left = {'py': q + 1}, {'py': q - 1}
    diag = p == q
    off_diag = jnp.logical_not(diag)
    asel = jnp.int32(1) * diag

    greet(p, q, True)
    load = pltpu.make_async_copy(z_ref, a_ref.at[:, 0:128, :], io.at[0])
    load.start()

    def rows_of(h):
        return pl.ds(pl.multiple_of(h * ROWS, ROWS), ROWS)

    def to_line(src, m, h, kind, dev):
        remote(src, col.at[m, rows_of(h)], ss.at[kind, m], rc.at[m, h], dev).start()

    def to_line_mask(src, m, kind, dev):
        remote(src, mc.at[m], sm.at[kind, m], rmc.at[m], dev).start()

    def plane(src, which, k, h, sem, rsem, dev):
        remote(src, zz.at[which, k, rows_of(h)], sem, rsem, dev).start()

    def own(h, first):
        part = zz.at[1, p, rows_of(h)]

        @pl.when(q < 3)
        def _():
            to_line(part, q, h, TO_RIGHT, right)
            if first is not None:
                pl.when(first)(lambda: to_line_mask(mm.at[1, p], q, TO_RIGHT, right))

        @pl.when(q > 0)
        def _():
            to_line(part, q, h, TO_LEFT, left)
            if first is not None:
                pl.when(first)(lambda: to_line_mask(mm.at[1, p], q, TO_LEFT, left))
        plane(part, 1, p, h, sp.at[0], rb.at[p, h], {'px': mirror})
        plane(part, 1, p, h, sp.at[1], rb.at[p, h], {'px': partner})
        if first is not None:
            @pl.when(first)
            def _():
                remote(mm.at[1, p], mm.at[1, p], spm.at[0], rmb.at[p], {'px': mirror}).start()
                remote(mm.at[1, p], mm.at[1, p], spm.at[1], rmb.at[p], {'px': partner}).start()

    mm[1, p] = mask_ref[...]
    load.wait()

    @pl.loop(0, chunks)
    def _(h):
        for r in range(ROWS):
            i = h * ROWS + r
            zt = a_ref[i, 0:128, :].astype(F32)
            zz[1, p, i] = norm_major(zt, li_ref[0], li_ref[1]).astype(BF16)

        @pl.when(h > 0)
        def _():
            own(h - 1, h == 1)

    @pl.loop(0, 128)
    def _(c):
        x_ref[c] = jnp.zeros((128, 128), F32)

    own(jnp.int32(chunks - 1), None)

    def pass_on(s, m, h):
        landed(col.at[m, rows_of(h)], rc.at[m, h])
        pl.when(h == 0)(lambda: landed(mc.at[m], rmc.at[m]))
        part = col.at[m, rows_of(h)]

        @pl.when(jnp.logical_and(q < 3, m < q))
        def _():
            to_line(part, m, h, TO_RIGHT, right)
            pl.when(h == 0)(lambda: to_line_mask(mc.at[m], m, TO_RIGHT, right))

        @pl.when(jnp.logical_and(q > 0, m > q))
        def _():
            to_line(part, m, h, TO_LEFT, left)
            pl.when(h == 0)(lambda: to_line_mask(mc.at[m], m, TO_LEFT, left))

        @pl.when(m != p)
        def _():
            plane(part, 0, p, h, ss.at[2, m], ra.at[p, h], {'px': m})
            pl.when(h == 0)(lambda: remote(mc.at[m], mm.at[0, p], sm.at[2, m], rma.at[p], {'px': m}).start())

        @pl.when(m == p)
        def _():
            pltpu.make_async_copy(part, zz.at[0, p, rows_of(h)], lc.at[h]).start()

            @pl.when(h == 0)
            def _():
                mm[0, p] = mc[p]

        @pl.when(s == 1)
        def _():
            landed(zz.at[1, mirror, rows_of(h)], rb.at[mirror, h])
            plane(zz.at[1, mirror, rows_of(h)], 1, mirror, h, sp.at[2], rb.at[mirror, h], {'px': partner})

            @pl.when(h == 0)
            def _():
                landed(mm.at[1, mirror], rmb.at[mirror])
                remote(mm.at[1, mirror], mm.at[1, mirror], spm.at[2], rmb.at[mirror], {'px': partner}).start()

    def compute(h):
        r0 = pl.multiple_of(h * ROWS, ROWS)

        @pl.loop(0, 4)
        def _(k):
            @pl.when(jnp.logical_and(k != p, k != mirror))
            def _():
                landed(zz.at[1, k, rows_of(h)], rb.at[k, h])
                pl.when(h == 0)(lambda: landed(mm.at[1, k], rmb.at[k]))

            @pl.when(jnp.logical_and(off_diag, k != p))
            def _():
                landed(zz.at[0, k, rows_of(h)], ra.at[k, h])
                pl.when(h == 0)(lambda: landed(mm.at[0, k], rma.at[k]))

            @pl.when(jnp.logical_and(off_diag, k == p))
            def _():
                landed(zz.at[0, k, rows_of(h)], lc.at[h])

            at = pl.multiple_of(k * 64 + lax.rem(h, 4) * ROWS, ROWS)
            mask_b = mm[1, k, pl.ds(r0, ROWS), :].astype(F32)
            project(lambda r: zz[1, k, r0 + r], mask_b, w_ref, b_ref, 256, stage, bb_ref, at)
            mask_a = mm[asel, k, pl.ds(r0, ROWS), :].astype(F32)
            project(lambda r: zz[asel, k, r0 + r], mask_a, w_ref, b_ref, 0, stage, a_ref, at)

        @pl.when(lax.rem(h, 4) == 3)
        def _():
            @pl.loop(0, 128 // 8)
            def _(n):
                for u in range(8):
                    c = n * 8 + u
                    x_ref[c] += lax.dot_general(a_ref[c], bb_ref[c], (((0,), (0,)), ((), ())), preferred_element_type=F32)

    third = 3 - 3 * lax.div(q, 2)
    second = 2 - lax.div(q, 2)
    last = p == third
    slot = jnp.where(p == second, 3, 2)

    @pl.loop(1, 4)
    def _(s):
        m = near_order(q, s)
        lag = jnp.where(last, 2, 0)
        when = jnp.where(last, 3, slot)

        @pl.loop(0, chunks + 2 * lax.div(s, 3))
        def _(h):
            @pl.when(h < chunks)
            def _():
                pass_on(s, m, h)

            @pl.when(jnp.logical_and(s == when, jnp.logical_and(h >= lag, h < chunks + lag)))
            def _():
                compute(h - lag)

    load.start()
    load.wait()

    def store(n):
        rows = pl.ds(pl.multiple_of(n * 8, 8), 8)
        return pltpu.make_async_copy(bb_ref.at[rows, 0:128, :], out_ref.at[rows], io.at[1])

    @pl.loop(0, 16)
    def _(n):
        def emit(i, value):
            bb_ref[i, 0:128, :] = jnp.transpose(value).astype(BF16)
        finish_rows(n, x_ref, lambda i: a_ref[i, 0:128, :], lambda i: zz[1, p, i], w_ref, b_ref, wo_ref, bo_ref, lo_ref, stage8, emit)
        pl.when(n > 0)(lambda: store(n - 1).start())

    store(jnp.int32(15)).start()

    for m in range(4):
        def drain(kind, when):
            @pl.when(when)
            def _():
                landed(col.at[m], ss.at[kind, m])
                landed(mc.at[m], sm.at[kind, m])
        drain(TO_RIGHT, jnp.logical_and(q < 3, m <= q))
        drain(TO_LEFT, jnp.logical_and(q > 0, m >= q))
        drain(2, jnp.logical_and(m != q, m != p))
    for kind in range(3):
        landed(zz.at[1, 0], sp.at[kind])
        landed(mm.at[1, 0], spm.at[kind])
    pltpu.make_async_copy(bb_ref.at[:, 0:128, :], out_ref, io.at[1]).wait()


def incoming(z, mask, wt, bias, ln_in, wo, bo, ln_out):
    n = 128 // ROWS
    return pl.pallas_call(
        incoming_kernel,
        out_shape=[jax.ShapeDtypeStruct((128, 128, 128), BF16), jax.ShapeDtypeStruct((4, 128, 128, 128), BF16)],
        in_specs=[ANY] + [VM] * 7,
        out_specs=[ANY, ANY],
        scratch_shapes=[
            pltpu.VMEM((2, 4, 128, 128, 128), BF16),
            pltpu.VMEM((2, 4, 128, 128), BF16),
            pltpu.VMEM((4, 128, 128), BF16),
            pltpu.VMEM((128, 256, 128), BF16),
            pltpu.VMEM((128, 256, 128), BF16),
            pltpu.VMEM((128, 128, 128), F32),
            pltpu.VMEM((ROWS, 128, 128), F32),
            pltpu.VMEM((8, 128, 128), F32),
            DMA((4, n)), DMA((4, n)), DMA((4, n)), DMA((n,)), DMA((4,)), DMA((4,)), DMA((4,)), DMA((2,)),
            DMA((3, 4)), DMA((3, 4)), DMA((3,)), DMA((3,)),
        ],
        compiler_params=pltpu.CompilerParams(collective_id=1, has_side_effects=True, vmem_limit_bytes=67043328),
        name='incoming',
    )(z, mask, wt, bias, ln_in, wo, bo, ln_out)[0]


def solution(mesh):
    pair_spec = P(('batch', 'px'), 'py', None)
    mask_spec = P(('batch', 'px'), 'py')
    whole = P()

    def device_body(pair_blk, mask_blk, ln_in, w_in, b_in, ln_out, w_out, b_out):
        mask = mask_blk.astype(BF16)
        wt = jnp.swapaxes(w_in, 1, 2)
        wo = jnp.swapaxes(w_out, 1, 2)
        def wide(v):
            return jnp.broadcast_to(v.astype(F32)[..., None], v.shape + (128,))
        bias, bo, li, lo = wide(b_in), wide(b_out), wide(ln_in), wide(ln_out)
        z1 = outgoing(pair_blk, mask, wt[0], bias[0], li[0], wo[0], bo[0], lo[0])
        return incoming(z1, mask, wt[1], bias[1], li[1], wo[1], bo[1], lo[1])

    return jax.shard_map(device_body, mesh=mesh, in_specs=(pair_spec, mask_spec, whole, whole, whole, whole, whole, whole), out_specs=pair_spec, check_vma=False)
```

```python
import functools

import jax
import jax.numpy as jnp
from jax import lax
from jax.experimental import pallas as pl
from jax.experimental.pallas import tpu as pltpu
from jax.sharding import PartitionSpec as P

LN_EPS = 1e-5
MESH = pl.DeviceIdType.MESH
F32, BF16 = jnp.float32, jnp.bfloat16
ROWS = 16
TO_RIGHT, TO_LEFT, TO_PARTNER, TO_MIRROR = 0, 1, 2, 3


def norm_major(values, gain, shift):
    average = jnp.mean(values, axis=0, keepdims=True)
    centered = values - average
    variance = jnp.mean(centered * centered, axis=0, keepdims=True)
    return centered * lax.rsqrt(variance + LN_EPS) * gain + shift


def remote(src, dst, send_sem, recv_sem, device):
    return pltpu.make_async_remote_copy(src_ref=src, dst_ref=dst, send_sem=send_sem, recv_sem=recv_sem, device_id=device, device_id_type=MESH)


def landed(ref, sem):
    pltpu.make_async_copy(ref, ref, sem).wait()


def project(rows, mask, w_ref, b_ref, base, stage, dst, at):
    w = w_ref[base:base + 256, :]
    for r in range(0, ROWS, 2):
        pair = jnp.concatenate([rows(r), rows(r + 1)], axis=1)
        prod = jnp.dot(w, pair, preferred_element_type=F32)
        for t in range(2):
            gate = prod[:128, 128 * t:128 * t + 128] + b_ref[base:base + 128, :]
            value = prod[128:, 128 * t:128 * t + 128] + b_ref[base + 128:base + 256, :]
            stage[r + t] = mask[r + t:r + t + 1] * jax.nn.sigmoid(gate) * value
    dst[:, pl.ds(at, ROWS), :] = jnp.transpose(stage[...], (1, 0, 2)).astype(BF16)


def finish_rows(n, x_ref, z_row, zn_row, w_ref, b_ref, wo_ref, bo_ref, lo_ref, stage, emit):
    i0 = pl.multiple_of(n * 8, 8)
    x = x_ref[:, pl.ds(i0, 8), :]
    average = jnp.mean(x, axis=0)
    centered = x - average[None]
    variance = jnp.mean(centered * centered, axis=0)
    scale = lax.rsqrt(variance + LN_EPS)
    stage[...] = jnp.transpose(centered * scale[None], (1, 0, 2))
    for r in range(0, 8, 2):
        pair = [(stage[r + t] * lo_ref[0] + lo_ref[1]).astype(BF16) for t in range(2)]
        update = jnp.dot(wo_ref[...], jnp.concatenate(pair, axis=1), preferred_element_type=F32)
        zn = jnp.concatenate([zn_row(i0 + r), zn_row(i0 + r + 1)], axis=1)
        gate = jnp.dot(w_ref[512:640, :], zn, preferred_element_type=F32)
        for t in range(2):
            lanes = slice(128 * t, 128 * t + 128)
            g = jax.nn.sigmoid(gate[:, lanes] + b_ref[512:640, :])
            emit(i0 + r + t, z_row(i0 + r + t).astype(F32) + g * (update[:, lanes] + bo_ref[...]))


def near_order(q, s, update):
    if update == 0:
        first, second = q + 1 - 2 * lax.rem(q, 2), 2 - lax.div(q, 2)
    else:
        first, second = 2 - lax.div(q, 2), q + 1 - 2 * lax.rem(q, 2)
    third = 3 - 3 * lax.div(q, 2)
    is0, is1, is2, is3 = (jnp.int32(1) * (s == v) for v in range(4))
    return is0 * q + is1 * first + is2 * second + is3 * third


def greet(p, q, everyone):
    barrier = pltpu.get_barrier_semaphore()
    peers = [lax.rem(p + d, 4) for d in (1, 2, 3)] if everyone else [p + 1 - 2 * lax.rem(p, 2), lax.rem(p + 2, 4)]
    for peer in peers:
        pl.semaphore_signal(barrier, inc=1, device_id={'px': peer}, device_id_type=MESH)

    @pl.when(q < 3)
    def _():
        pl.semaphore_signal(barrier, inc=1, device_id={'py': q + 1}, device_id_type=MESH)

    @pl.when(q > 0)
    def _():
        pl.semaphore_signal(barrier, inc=1, device_id={'py': q - 1}, device_id_type=MESH)

    edge = jnp.int32(1) * (q == 0) + jnp.int32(1) * (q == 3)
    pl.semaphore_wait(barrier, len(peers) + 2 - edge)


def kernel(z_ref, mask_ref, li_in, w_in, b_in, lo_in, wo_in, bo_in, out_ref, col, keep,
           w_refs, b_refs, li_refs, wo_refs, bo_refs, lo_refs, zz, mb, mm, mc, a_ref, bb_ref, x_ref, stage, stage8,
           ra1, rb1, rma1, rmb1, ss1, sm1, rc, ra, rb, lc, rmc, rma, rmb, io, ss, sm, sp, spm, free):
    chunks = 128 // ROWS
    p, q = lax.axis_index('px'), lax.axis_index('py')
    partner, mirror = p + 1 - 2 * lax.rem(p, 2), lax.rem(p + 2, 4)
    right, left = {'py': q + 1}, {'py': q - 1}
    diag = p == q
    off_diag = jnp.logical_not(diag)
    relay = p == lax.rem(q + 2, 4)
    asel = jnp.int32(1) * diag
    bsel = 1 - asel
    plane_peers = [lax.rem(p + d, 4) for d in (1, 2, 3)]

    greet(p, q, True)
    load = pltpu.make_async_copy(z_ref, bb_ref.at[:, 128:256, :], io.at[0])
    load.start()

    def rows_of(h):
        return pl.ds(pl.multiple_of(h * ROWS, ROWS), ROWS)

    w_ref, b_ref, li_ref, wo_ref, bo_ref, lo_ref = (r.at[0] for r in (w_refs, b_refs, li_refs, wo_refs, bo_refs, lo_refs))
    zb = zz

    def along(k, h, kind, dev):
        part = zb.at[0, k, rows_of(h)]
        remote(part, part, ss1.at[kind, k], ra1.at[k, h], dev).start()

    def across(which, k, h, kind, dev):
        remote(zb.at[which, k, rows_of(h)], zb.at[1, k, rows_of(h)], ss1.at[kind, k], rb1.at[k, h], dev).start()

    def along_mask(k, kind, dev):
        remote(mb.at[0, k], mb.at[0, k], sm1.at[kind, k], rma1.at[k], dev).start()

    def across_mask(which, k, kind, dev):
        remote(mb.at[which, k], mb.at[1, k], sm1.at[kind, k], rmb1.at[k], dev).start()

    def spread(k, h, first):
        @pl.when(jnp.logical_and(q < 3, k <= q))
        def _():
            along(k, h, TO_RIGHT, right)
            if first is not None:
                pl.when(first)(lambda: along_mask(k, TO_RIGHT, right))

        @pl.when(jnp.logical_and(q > 0, k >= q))
        def _():
            along(k, h, TO_LEFT, left)
            if first is not None:
                pl.when(first)(lambda: along_mask(k, TO_LEFT, left))

        @pl.when(diag)
        def _():
            across(0, k, h, TO_MIRROR, {'px': mirror})
            across(0, k, h, TO_PARTNER, {'px': partner})
            if first is not None:
                @pl.when(first)
                def _():
                    across_mask(0, k, TO_MIRROR, {'px': mirror})
                    across_mask(0, k, TO_PARTNER, {'px': partner})

    mask = mask_ref[...].astype(F32).astype(BF16)
    mb[0, q] = mask
    mm[1, p] = mask

    def wide(row):
        return jnp.transpose(jnp.broadcast_to(row.astype(F32), (128, 128)))

    for u in range(2):
        ln_rows = li_in[u].astype(F32)
        for t in range(2):
            li_refs[u, t] = wide(ln_rows[t:t + 1])
    load.wait()

    @pl.loop(0, chunks)
    def _(h):
        for r in range(ROWS):
            i = h * ROWS + r
            zt = jnp.transpose(bb_ref[i, 128:256, :].astype(F32))
            a_ref[i, 128:256, :] = zt.astype(BF16)
            zb[0, q, i] = norm_major(zt, li_ref[0], li_ref[1]).astype(BF16)

        @pl.when(h > 0)
        def _():
            spread(q, h - 1, h == 1)

    @pl.loop(0, 128)
    def _(c):
        x_ref[c] = jnp.zeros((128, 128), F32)

    spread(q, jnp.int32(chunks - 1), None)

    b_rows, bo_rows = b_in[...].astype(F32), bo_in[...].astype(F32)
    for u in range(2):
        lo_rows = lo_in[u].astype(F32)
        for t in range(2):
            lo_refs[u, t] = wide(lo_rows[t:t + 1])
        bo_refs[u] = wide(bo_rows[u:u + 1])
        wo_refs[u] = jnp.transpose(wo_in[u].astype(F32)).astype(BF16)
        for e in range(0, 640, 128):
            b_refs[u, e:e + 128, :] = wide(b_rows[u:u + 1, e:e + 128])
            w_refs[u, e:e + 128, :] = jnp.transpose(w_in[u, :, e:e + 128].astype(F32)).astype(BF16)

    @pl.loop(0, 4)
    def _(s):
        k = near_order(q, s, 0)

        @pl.loop(0, chunks)
        def _(h):
            @pl.when(s > 0)
            def _():
                landed(zb.at[0, k, rows_of(h)], ra1.at[k, h])
                pl.when(h == 0)(lambda: landed(mb.at[0, k], rma1.at[k]))
                spread(k, h, h == 0)

            @pl.when(jnp.logical_not(diag))
            def _():
                landed(zb.at[1, k, rows_of(h)], rb1.at[k, h])
                pl.when(h == 0)(lambda: landed(mb.at[1, k], rmb1.at[k]))

                @pl.when(relay)
                def _():
                    across(1, k, h, TO_PARTNER, {'px': partner})
                    pl.when(h == 0)(lambda: across_mask(1, k, TO_PARTNER, {'px': partner}))

            r0 = pl.multiple_of(h * ROWS, ROWS)
            mask_a = mb[0, k, pl.ds(r0, ROWS), :].astype(F32)
            project(lambda r: zb[0, k, r0 + r], mask_a, w_ref, b_ref, 0, stage, a_ref, r0)
            mask_b = mb[bsel, k, pl.ds(r0, ROWS), :].astype(F32)
            project(lambda r: zb[bsel, k, r0 + r], mask_b, w_ref, b_ref, 256, stage, bb_ref, r0)

        @pl.loop(0, 128 // 16)
        def _(n):
            for u in range(16):
                c = n * 16 + u
                x_ref[c] += lax.dot_general(a_ref[c, 0:128, :], bb_ref[c, 0:128, :], (((1,), (1,)), ((), ())), preferred_element_type=F32)

    def to_line(src, m, h, kind, dev):
        remote(src, col.at[m, rows_of(h)], ss.at[kind, m], rc.at[m, h], dev).start()

    def to_line_mask(src, m, kind, dev):
        remote(src, mc.at[m], sm.at[kind, m], rmc.at[m], dev).start()

    def plane(src, which, k, h, sem, rsem, dev):
        remote(src, zz.at[which, k, rows_of(h)], sem, rsem, dev).start()

    def own_line(h, first):
        part = zz.at[1, p, rows_of(h)]

        @pl.when(jnp.logical_and(q < 3, q != 2))
        def _():
            to_line(part, q, h, TO_RIGHT, right)
            pl.when(first)(lambda: to_line_mask(mm.at[1, p], q, TO_RIGHT, right))

        @pl.when(jnp.logical_and(q > 0, q != 1))
        def _():
            to_line(part, q, h, TO_LEFT, left)
            pl.when(first)(lambda: to_line_mask(mm.at[1, p], q, TO_LEFT, left))

        @pl.when(first)
        def _():
            pl.semaphore_wait(free.at[0], 3)
            remote(mm.at[1, p], mm.at[1, p], spm.at[0], rmb.at[p], {'px': mirror}).start()
            remote(mm.at[1, p], mm.at[1, p], spm.at[1], rmb.at[p], {'px': partner}).start()
        plane(part, 1, p, h, sp.at[0], rb.at[p, h], {'px': mirror})
        plane(part, 1, p, h, sp.at[1], rb.at[p, h], {'px': partner})

    @pl.when(relay)
    def _():
        for k in range(4):
            landed(zz.at[1, k], ss1.at[TO_PARTNER, k])
            landed(mb.at[1, k], sm1.at[TO_PARTNER, k])
    for peer in plane_peers:
        pl.semaphore_signal(free.at[0], inc=1, device_id={'px': peer}, device_id_type=MESH)

    @pl.loop(0, 16)
    def _(n):
        def emit(i, value):
            z1 = value.astype(BF16)
            a_ref[i, 128:256, :] = z1
            zz[1, p, i] = norm_major(z1.astype(F32), li_refs[1, 0], li_refs[1, 1]).astype(BF16)
        finish_rows(n, x_ref, lambda i: a_ref[i, 128:256, :], lambda i: zz[0, q, i], w_ref, b_ref, wo_ref, bo_ref, lo_ref, stage8, emit)

        @pl.when(jnp.logical_and(n > 1, lax.rem(n, 2) == 0))
        def _():
            own_line(lax.div(n, 2) - 1, n == 2)

    save = pltpu.make_async_copy(a_ref.at[:, 128:256, :], keep, io.at[0])
    save.start()

    w_ref, b_ref, wo_ref, bo_ref, lo_ref = (r.at[1] for r in (w_refs, b_refs, wo_refs, bo_refs, lo_refs))

    @pl.loop(0, 128)
    def _(c):
        x_ref[c] = jnp.zeros((128, 128), F32)

    own_line(jnp.int32(chunks - 1), jnp.bool_(False))
    save.wait()
    for k in range(4):
        def drain0(kind, when):
            @pl.when(when)
            def _():
                landed(zz.at[0, k], ss1.at[kind, k])
                landed(mb.at[0, k], sm1.at[kind, k])
        drain0(TO_RIGHT, jnp.logical_and(q < 3, k <= q))
        drain0(TO_LEFT, jnp.logical_and(q > 0, k >= q))
        drain0(TO_MIRROR, diag)
        drain0(TO_PARTNER, diag)
    for peer in plane_peers:
        pl.semaphore_signal(free.at[1], inc=1, device_id={'px': peer}, device_id_type=MESH)
    pl.semaphore_wait(free.at[1], 3)

    def pass_on(s, m, h):
        landed(col.at[m, rows_of(h)], rc.at[m, h])
        pl.when(h == 0)(lambda: landed(mc.at[m], rmc.at[m]))
        part = col.at[m, rows_of(h)]

        @pl.when(jnp.logical_and(q < 3, m < q))
        def _():
            to_line(part, m, h, TO_RIGHT, right)
            pl.when(h == 0)(lambda: to_line_mask(mc.at[m], m, TO_RIGHT, right))

        @pl.when(jnp.logical_and(q > 0, m > q))
        def _():
            to_line(part, m, h, TO_LEFT, left)
            pl.when(h == 0)(lambda: to_line_mask(mc.at[m], m, TO_LEFT, left))

        @pl.when(m != p)
        def _():
            plane(part, 0, p, h, ss.at[2, m], ra.at[p, h], {'px': m})
            pl.when(h == 0)(lambda: remote(mc.at[m], mm.at[0, p], sm.at[2, m], rma.at[p], {'px': m}).start())

        @pl.when(m == p)
        def _():
            pltpu.make_async_copy(part, zz.at[0, p, rows_of(h)], lc.at[h]).start()

            @pl.when(h == 0)
            def _():
                mm[0, p] = mc[p]

        @pl.when(s == 1)
        def _():
            landed(zz.at[1, mirror, rows_of(h)], rb.at[mirror, h])
            plane(zz.at[1, mirror, rows_of(h)], 1, mirror, h, sp.at[2], rb.at[mirror, h], {'px': partner})

            @pl.when(h == 0)
            def _():
                landed(mm.at[1, mirror], rmb.at[mirror])
                remote(mm.at[1, mirror], mm.at[1, mirror], spm.at[2], rmb.at[mirror], {'px': partner}).start()

    def compute(h):
        r0 = pl.multiple_of(h * ROWS, ROWS)

        @pl.loop(0, 4)
        def _(k):
            @pl.when(jnp.logical_and(k != p, k != mirror))
            def _():
                landed(zz.at[1, k, rows_of(h)], rb.at[k, h])
                pl.when(h == 0)(lambda: landed(mm.at[1, k], rmb.at[k]))

            @pl.when(jnp.logical_and(off_diag, k != p))
            def _():
                landed(zz.at[0, k, rows_of(h)], ra.at[k, h])
                pl.when(h == 0)(lambda: landed(mm.at[0, k], rma.at[k]))

            @pl.when(jnp.logical_and(off_diag, k == p))
            def _():
                landed(zz.at[0, k, rows_of(h)], lc.at[h])

            at = pl.multiple_of(k * 64 + lax.rem(h, 4) * ROWS, ROWS)
            mask_b = mm[1, k, pl.ds(r0, ROWS), :].astype(F32)
            project(lambda r: zz[1, k, r0 + r], mask_b, w_ref, b_ref, 256, stage, bb_ref, at)
            mask_a = mm[asel, k, pl.ds(r0, ROWS), :].astype(F32)
            project(lambda r: zz[asel, k, r0 + r], mask_a, w_ref, b_ref, 0, stage, a_ref, at)

        @pl.when(lax.rem(h, 4) == 3)
        def _():
            @pl.loop(0, 128 // 8)
            def _(n):
                for u in range(8):
                    c = n * 8 + u
                    x_ref[c] += lax.dot_general(a_ref[c], bb_ref[c], (((0,), (0,)), ((), ())), preferred_element_type=F32)

    third = 3 - 3 * lax.div(q, 2)
    second = q + 1 - 2 * lax.rem(q, 2)
    last = p == third
    slot = jnp.where(p == second, 3, 2)

    @pl.loop(1, 4)
    def _(s):
        m = near_order(q, s, 1)
        lag = jnp.where(last, 2, 0)
        when = jnp.where(last, 3, slot)

        @pl.loop(0, chunks + 2 * lax.div(s, 3))
        def _(h):
            @pl.when(h < chunks)
            def _():
                pass_on(s, m, h)

            @pl.when(jnp.logical_and(s == when, jnp.logical_and(h >= lag, h < chunks + lag)))
            def _():
                compute(h - lag)

        @pl.when(jnp.logical_and(s == 1, lax.rem(q, 3) > 0))
        def _():
            to_line_mask(mm.at[1, p], q, 2 - q, {'py': 3 * (q - 1)})

            @pl.loop(0, chunks)
            def _(h):
                to_line(zz.at[1, p, rows_of(h)], q, h, 2 - q, {'py': 3 * (q - 1)})

    load = pltpu.make_async_copy(keep, a_ref.at[:, 0:128, :], io.at[0])
    load.start()
    load.wait()

    def store(n):
        rows = pl.ds(pl.multiple_of(n * 8, 8), 8)
        return pltpu.make_async_copy(bb_ref.at[rows, 0:128, :], out_ref.at[rows], io.at[1])

    @pl.loop(0, 16)
    def _(n):
        def emit(i, value):
            bb_ref[i, 0:128, :] = jnp.transpose(value).astype(BF16)
        finish_rows(n, x_ref, lambda i: a_ref[i, 0:128, :], lambda i: zz[1, p, i], w_ref, b_ref, wo_ref, bo_ref, lo_ref, stage8, emit)
        pl.when(n > 0)(lambda: store(n - 1).start())

    store(jnp.int32(15)).start()

    for m in range(4):
        def drain(kind, when):
            @pl.when(when)
            def _():
                landed(col.at[m], ss.at[kind, m])
                landed(mc.at[m], sm.at[kind, m])
        drain(TO_RIGHT, jnp.logical_and(q < 3, m <= q))
        drain(TO_LEFT, jnp.logical_and(q > 0, m >= q))
        drain(2, jnp.logical_and(m != q, m != p))
    for kind in range(3):
        landed(zz.at[1, 0], sp.at[kind])
        landed(mm.at[1, 0], spm.at[kind])
    pltpu.make_async_copy(bb_ref.at[:, 0:128, :], out_ref, io.at[1]).wait()


VM = pl.BlockSpec(memory_space=pltpu.VMEM)
ANY = pl.BlockSpec(memory_space=pl.ANY)
DMA = pltpu.SemaphoreType.DMA


def both_updates(*args):
    n = 128 // ROWS
    block = jax.ShapeDtypeStruct((128, 128, 128), BF16)
    return pl.pallas_call(
        kernel,
        out_shape=[block, jax.ShapeDtypeStruct((4, 128, 128, 128), BF16), block],
        in_specs=[ANY] + [VM] * 7,
        out_specs=[ANY, ANY, ANY],
        scratch_shapes=[
            pltpu.VMEM((2, 640, 128), BF16),
            pltpu.VMEM((2, 640, 128), F32),
            pltpu.VMEM((2, 2, 128, 128), F32),
            pltpu.VMEM((2, 128, 128), BF16),
            pltpu.VMEM((2, 128, 128), F32),
            pltpu.VMEM((2, 2, 128, 128), F32),
            pltpu.VMEM((2, 4, 128, 128, 128), BF16),
            pltpu.VMEM((2, 4, 128, 128), BF16),
            pltpu.VMEM((2, 4, 128, 128), BF16),
            pltpu.VMEM((4, 128, 128), BF16),
            pltpu.VMEM((128, 256, 128), BF16),
            pltpu.VMEM((128, 256, 128), BF16),
            pltpu.VMEM((128, 128, 128), F32),
            pltpu.VMEM((ROWS, 128, 128), F32),
            pltpu.VMEM((8, 128, 128), F32),
            DMA((4, n)), DMA((4, n)), DMA((4,)), DMA((4,)), DMA((4, 4)), DMA((4, 4)),
            DMA((4, n)), DMA((4, n)), DMA((4, n)), DMA((n,)), DMA((4,)), DMA((4,)), DMA((4,)), DMA((2,)),
            DMA((3, 4)), DMA((3, 4)), DMA((3,)), DMA((3,)),
            pltpu.SemaphoreType.REGULAR((2,)),
        ],
        compiler_params=pltpu.CompilerParams(collective_id=0, has_side_effects=True, vmem_limit_bytes=67043328),
        name='both_updates',
    )(*args)[0]


def solution(mesh):
    pair_spec = P(('batch', 'px'), 'py', None)
    mask_spec = P(('batch', 'px'), 'py')
    whole = P()

    return jax.shard_map(both_updates, mesh=mesh, in_specs=(pair_spec, mask_spec, whole, whole, whole, whole, whole, whole), out_specs=pair_spec, check_vma=False)
```

```python
import functools

import jax
import jax.numpy as jnp
from jax import lax
from jax.experimental import pallas as pl
from jax.experimental.pallas import tpu as pltpu
from jax.sharding import PartitionSpec as P

LN_EPS = 1e-5
MESH = pl.DeviceIdType.MESH
F32, BF16 = jnp.float32, jnp.bfloat16
ROWS = 16
TO_RIGHT, TO_LEFT, TO_PARTNER, TO_MIRROR = 0, 1, 2, 3


def norm_major(values, gain, shift):
    average = jnp.mean(values, axis=0, keepdims=True)
    centered = values - average
    variance = jnp.mean(centered * centered, axis=0, keepdims=True)
    return centered * lax.rsqrt(variance + LN_EPS) * gain + shift


def remote(src, dst, send_sem, recv_sem, device):
    return pltpu.make_async_remote_copy(src_ref=src, dst_ref=dst, send_sem=send_sem, recv_sem=recv_sem, device_id=device, device_id_type=MESH)


def landed(ref, sem):
    pltpu.make_async_copy(ref, ref, sem).wait()


def project(rows, mask, w_ref, b_ref, base, stage, dst, at):
    w = w_ref[base:base + 256, :]
    for r in range(0, ROWS, 2):
        pair = jnp.concatenate([rows(r), rows(r + 1)], axis=1)
        prod = jnp.dot(w, pair, preferred_element_type=F32)
        for t in range(2):
            gate = prod[:128, 128 * t:128 * t + 128] + b_ref[base:base + 128, :]
            value = prod[128:, 128 * t:128 * t + 128] + b_ref[base + 128:base + 256, :]
            stage[r + t] = mask[r + t:r + t + 1] * jax.nn.sigmoid(gate) * value
    dst[:, pl.ds(at, ROWS), :] = jnp.transpose(stage[...], (1, 0, 2)).astype(BF16)


def finish_rows(n, x_ref, z_row, zn_row, w_ref, b_ref, wo_ref, bo_ref, lo_ref, stage, emit):
    i0 = pl.multiple_of(n * ROWS, ROWS)
    for r in range(0, ROWS, 8):
        x = x_ref[:, pl.ds(i0 + r, 8), :]
        average = jnp.mean(x, axis=0)
        centered = x - average[None]
        variance = jnp.mean(centered * centered, axis=0)
        scale = lax.rsqrt(variance + LN_EPS)
        stage[r:r + 8] = jnp.transpose(centered * scale[None], (1, 0, 2))
    for r in range(0, ROWS, 2):
        pair = [(stage[r + t] * lo_ref[0] + lo_ref[1]).astype(BF16) for t in range(2)]
        update = jnp.dot(wo_ref[...], jnp.concatenate(pair, axis=1), preferred_element_type=F32)
        zn = jnp.concatenate([zn_row(i0 + r), zn_row(i0 + r + 1)], axis=1)
        gate = jnp.dot(w_ref[512:640, :], zn, preferred_element_type=F32)
        for t in range(2):
            lanes = slice(128 * t, 128 * t + 128)
            g = jax.nn.sigmoid(gate[:, lanes] + b_ref[512:640, :])
            emit(i0 + r + t, z_row(i0 + r + t).astype(F32) + g * (update[:, lanes] + bo_ref[...]))


def near_order(q, s, update):
    if update == 0:
        first, second = q + 1 - 2 * lax.rem(q, 2), 2 - lax.div(q, 2)
    else:
        first, second = 2 - lax.div(q, 2), q + 1 - 2 * lax.rem(q, 2)
    third = 3 - 3 * lax.div(q, 2)
    is0, is1, is2, is3 = (jnp.int32(1) * (s == v) for v in range(4))
    return is0 * q + is1 * first + is2 * second + is3 * third


def greet(p, q, everyone):
    barrier = pltpu.get_barrier_semaphore()
    peers = [lax.rem(p + d, 4) for d in (1, 2, 3)] if everyone else [p + 1 - 2 * lax.rem(p, 2), lax.rem(p + 2, 4)]
    for peer in peers:
        pl.semaphore_signal(barrier, inc=1, device_id={'px': peer}, device_id_type=MESH)

    @pl.when(q < 3)
    def _():
        pl.semaphore_signal(barrier, inc=1, device_id={'py': q + 1}, device_id_type=MESH)

    @pl.when(q > 0)
    def _():
        pl.semaphore_signal(barrier, inc=1, device_id={'py': q - 1}, device_id_type=MESH)

    edge = jnp.int32(1) * (q == 0) + jnp.int32(1) * (q == 3)
    return lambda: pl.semaphore_wait(barrier, len(peers) + 2 - edge)


def kernel(z_ref, mask_ref, li_in, w_in, b_in, lo_in, wo_in, bo_in, out_ref, col, keep,
           w_refs, b_refs, li_refs, wo_refs, bo_refs, lo_refs, zz, mb, mm, mc, a_ref, bb_ref, x_ref, stage,
           ra1, rb1, rma1, rmb1, ss1, sm1, rc, ra, rb, lc, rmc, rma, rmb, io, ss, sm, sp, spm, free):
    chunks = 128 // ROWS
    p, q = lax.axis_index('px'), lax.axis_index('py')
    partner, mirror = p + 1 - 2 * lax.rem(p, 2), lax.rem(p + 2, 4)
    right, left = {'py': q + 1}, {'py': q - 1}
    diag = p == q
    off_diag = jnp.logical_not(diag)
    relay = p == lax.rem(q + 2, 4)
    asel = jnp.int32(1) * diag
    bsel = 1 - asel
    plane_peers = [lax.rem(p + d, 4) for d in (1, 2, 3)]

    met = greet(p, q, True)
    load_first = pltpu.make_async_copy(z_ref.at[0:ROWS], bb_ref.at[0:ROWS, 128:256, :], io.at[0])
    load_rest = pltpu.make_async_copy(z_ref.at[ROWS:128], bb_ref.at[ROWS:128, 128:256, :], io.at[1])
    load_first.start()
    load_rest.start()

    def rows_of(h):
        return pl.ds(pl.multiple_of(h * ROWS, ROWS), ROWS)

    w_ref, b_ref, li_ref, wo_ref, bo_ref, lo_ref = (r.at[0] for r in (w_refs, b_refs, li_refs, wo_refs, bo_refs, lo_refs))
    zb = zz

    def along(k, h, kind, dev):
        part = zb.at[0, k, rows_of(h)]
        remote(part, part, ss1.at[kind, k], ra1.at[k, h], dev).start()

    def across(which, k, h, kind, dev):
        remote(zb.at[which, k, rows_of(h)], zb.at[1, k, rows_of(h)], ss1.at[kind, k], rb1.at[k, h], dev).start()

    def along_mask(k, kind, dev):
        remote(mb.at[0, k], mb.at[0, k], sm1.at[kind, k], rma1.at[k], dev).start()

    def across_mask(which, k, kind, dev):
        remote(mb.at[which, k], mb.at[1, k], sm1.at[kind, k], rmb1.at[k], dev).start()

    def spread(k, h, first):
        @pl.when(jnp.logical_and(q < 3, k <= q))
        def _():
            along(k, h, TO_RIGHT, right)
            if first is not None:
                pl.when(first)(lambda: along_mask(k, TO_RIGHT, right))

        @pl.when(jnp.logical_and(q > 0, k >= q))
        def _():
            along(k, h, TO_LEFT, left)
            if first is not None:
                pl.when(first)(lambda: along_mask(k, TO_LEFT, left))

        @pl.when(diag)
        def _():
            across(0, k, h, TO_MIRROR, {'px': mirror})
            across(0, k, h, TO_PARTNER, {'px': partner})
            if first is not None:
                @pl.when(first)
                def _():
                    across_mask(0, k, TO_MIRROR, {'px': mirror})
                    across_mask(0, k, TO_PARTNER, {'px': partner})

    mask = mask_ref[...].astype(F32).astype(BF16)
    mb[0, q] = mask
    mm[1, p] = mask

    def wide(row):
        return jnp.transpose(jnp.broadcast_to(row.astype(F32), (128, 128)))

    for u in range(2):
        ln_rows = li_in[u].astype(F32)
        for t in range(2):
            li_refs[u, t] = wide(ln_rows[t:t + 1])
    def prepare(h):
        for r in range(ROWS):
            i = h * ROWS + r
            zt = jnp.transpose(bb_ref[i, 128:256, :].astype(F32))
            a_ref[i, 128:256, :] = zt.astype(BF16)
            zb[0, q, i] = norm_major(zt, li_ref[0], li_ref[1]).astype(BF16)

    load_first.wait()
    prepare(0)
    met()
    load_rest.wait()

    @pl.loop(1, chunks)
    def _(h):
        prepare(h)
        spread(q, h - 1, h == 1)

    @pl.loop(0, 128)
    def _(c):
        x_ref[c] = jnp.zeros((128, 128), F32)

    spread(q, jnp.int32(chunks - 1), None)

    b_rows, bo_rows = b_in[...].astype(F32), bo_in[...].astype(F32)
    for u in range(2):
        lo_rows = lo_in[u].astype(F32)
        for t in range(2):
            lo_refs[u, t] = wide(lo_rows[t:t + 1])
        bo_refs[u] = wide(bo_rows[u:u + 1])
        wo_refs[u] = jnp.transpose(wo_in[u].astype(F32)).astype(BF16)
        for e in range(0, 640, 128):
            b_refs[u, e:e + 128, :] = wide(b_rows[u:u + 1, e:e + 128])
            w_refs[u, e:e + 128, :] = jnp.transpose(w_in[u, :, e:e + 128].astype(F32)).astype(BF16)

    @pl.loop(0, 4)
    def _(s):
        k = near_order(q, s, 0)

        @pl.loop(0, chunks)
        def _(h):
            @pl.when(s > 0)
            def _():
                landed(zb.at[0, k, rows_of(h)], ra1.at[k, h])
                pl.when(h == 0)(lambda: landed(mb.at[0, k], rma1.at[k]))
                spread(k, h, h == 0)

            @pl.when(jnp.logical_not(diag))
            def _():
                landed(zb.at[1, k, rows_of(h)], rb1.at[k, h])
                pl.when(h == 0)(lambda: landed(mb.at[1, k], rmb1.at[k]))

                @pl.when(relay)
                def _():
                    across(1, k, h, TO_PARTNER, {'px': partner})
                    pl.when(h == 0)(lambda: across_mask(1, k, TO_PARTNER, {'px': partner}))

            r0 = pl.multiple_of(h * ROWS, ROWS)
            mask_a = mb[0, k, pl.ds(r0, ROWS), :].astype(F32)
            project(lambda r: zb[0, k, r0 + r], mask_a, w_ref, b_ref, 0, stage, a_ref, r0)
            mask_b = mb[bsel, k, pl.ds(r0, ROWS), :].astype(F32)
            project(lambda r: zb[bsel, k, r0 + r], mask_b, w_ref, b_ref, 256, stage, bb_ref, r0)

        @pl.loop(0, 128 // 16)
        def _(n):
            for u in range(16):
                c = n * 16 + u
                x_ref[c] += lax.dot_general(a_ref[c, 0:128, :], bb_ref[c, 0:128, :], (((1,), (1,)), ((), ())), preferred_element_type=F32)

    def to_line(src, m, h, kind, dev):
        remote(src, col.at[m, rows_of(h)], ss.at[kind, m], rc.at[m, h], dev).start()

    def to_line_mask(src, m, kind, dev):
        remote(src, mc.at[m], sm.at[kind, m], rmc.at[m], dev).start()

    def plane(src, which, k, h, sem, rsem, dev):
        remote(src, zz.at[which, k, rows_of(h)], sem, rsem, dev).start()

    def own_line(h, first):
        part = zz.at[1, p, rows_of(h)]

        @pl.when(jnp.logical_and(q < 3, q != 2))
        def _():
            to_line(part, q, h, TO_RIGHT, right)
            pl.when(first)(lambda: to_line_mask(mm.at[1, p], q, TO_RIGHT, right))

        @pl.when(jnp.logical_and(q > 0, q != 1))
        def _():
            to_line(part, q, h, TO_LEFT, left)
            pl.when(first)(lambda: to_line_mask(mm.at[1, p], q, TO_LEFT, left))

        @pl.when(first)
        def _():
            pl.semaphore_wait(free.at[0], 3)
            remote(mm.at[1, p], mm.at[1, p], spm.at[0], rmb.at[p], {'px': mirror}).start()
            remote(mm.at[1, p], mm.at[1, p], spm.at[1], rmb.at[p], {'px': partner}).start()
        plane(part, 1, p, h, sp.at[0], rb.at[p, h], {'px': mirror})
        plane(part, 1, p, h, sp.at[1], rb.at[p, h], {'px': partner})

    @pl.when(relay)
    def _():
        for k in range(4):
            landed(zz.at[1, k], ss1.at[TO_PARTNER, k])
            landed(mb.at[1, k], sm1.at[TO_PARTNER, k])
    for peer in plane_peers:
        pl.semaphore_signal(free.at[0], inc=1, device_id={'px': peer}, device_id_type=MESH)

    @pl.loop(0, chunks)
    def _(n):
        def emit(i, value):
            z1 = value.astype(BF16)
            a_ref[i, 128:256, :] = z1
            zz[1, p, i] = norm_major(z1.astype(F32), li_refs[1, 0], li_refs[1, 1]).astype(BF16)
        finish_rows(n, x_ref, lambda i: a_ref[i, 128:256, :], lambda i: zz[0, q, i], w_ref, b_ref, wo_ref, bo_ref, lo_ref, stage, emit)

        @pl.when(n > 0)
        def _():
            own_line(n - 1, n == 1)

    save = pltpu.make_async_copy(a_ref.at[:, 128:256, :], keep, io.at[0])
    save.start()

    w_ref, b_ref, wo_ref, bo_ref, lo_ref = (r.at[1] for r in (w_refs, b_refs, wo_refs, bo_refs, lo_refs))

    @pl.loop(0, 128)
    def _(c):
        x_ref[c] = jnp.zeros((128, 128), F32)

    own_line(jnp.int32(chunks - 1), jnp.bool_(False))
    inner = lax.rem(q, 3) > 0

    @pl.when(inner)
    def _():
        m = near_order(q, jnp.int32(1), 1)
        kind, outer = 2 - q, {'py': 3 * (q - 1)}
        landed(mc.at[m], rmc.at[m])
        to_line_mask(mc.at[m], m, kind, outer)

        @pl.loop(0, chunks)
        def _(h):
            landed(col.at[m, rows_of(h)], rc.at[m, h])
            to_line(col.at[m, rows_of(h)], m, h, kind, outer)
        to_line_mask(mm.at[1, p], q, kind, outer)

        @pl.loop(0, chunks)
        def _(h):
            to_line(zz.at[1, p, rows_of(h)], q, h, kind, outer)

    save.wait()
    for k in range(4):
        def drain0(kind, when):
            @pl.when(when)
            def _():
                landed(zz.at[0, k], ss1.at[kind, k])
                landed(mb.at[0, k], sm1.at[kind, k])
        drain0(TO_RIGHT, jnp.logical_and(q < 3, k <= q))
        drain0(TO_LEFT, jnp.logical_and(q > 0, k >= q))
        drain0(TO_MIRROR, diag)
        drain0(TO_PARTNER, diag)
    for peer in plane_peers:
        pl.semaphore_signal(free.at[1], inc=1, device_id={'px': peer}, device_id_type=MESH)
    pl.semaphore_wait(free.at[1], 3)

    def pass_on(s, m, h):
        @pl.when(jnp.logical_or(s > 1, lax.rem(q, 3) == 0))
        def _():
            landed(col.at[m, rows_of(h)], rc.at[m, h])
            pl.when(h == 0)(lambda: landed(mc.at[m], rmc.at[m]))
        part = col.at[m, rows_of(h)]

        @pl.when(jnp.logical_and(s > 1, jnp.logical_and(q < 3, m < q)))
        def _():
            to_line(part, m, h, TO_RIGHT, right)
            pl.when(h == 0)(lambda: to_line_mask(mc.at[m], m, TO_RIGHT, right))

        @pl.when(jnp.logical_and(s > 1, jnp.logical_and(q > 0, m > q)))
        def _():
            to_line(part, m, h, TO_LEFT, left)
            pl.when(h == 0)(lambda: to_line_mask(mc.at[m], m, TO_LEFT, left))

        @pl.when(m != p)
        def _():
            plane(part, 0, p, h, ss.at[2, m], ra.at[p, h], {'px': m})
            pl.when(h == 0)(lambda: remote(mc.at[m], mm.at[0, p], sm.at[2, m], rma.at[p], {'px': m}).start())

        @pl.when(m == p)
        def _():
            pltpu.make_async_copy(part, zz.at[0, p, rows_of(h)], lc.at[h]).start()

            @pl.when(h == 0)
            def _():
                mm[0, p] = mc[p]

        @pl.when(s == 1)
        def _():
            landed(zz.at[1, mirror, rows_of(h)], rb.at[mirror, h])
            plane(zz.at[1, mirror, rows_of(h)], 1, mirror, h, sp.at[2], rb.at[mirror, h], {'px': partner})

            @pl.when(h == 0)
            def _():
                landed(mm.at[1, mirror], rmb.at[mirror])
                remote(mm.at[1, mirror], mm.at[1, mirror], spm.at[2], rmb.at[mirror], {'px': partner}).start()

    def group_row(k, h):
        return pl.multiple_of(lax.rem(h, 4) * 64 + k * ROWS, ROWS)

    def compute(h):
        @pl.when(lax.rem(h, 4) == 0)
        def _():
            @pl.loop(0, 16)
            def _(t):
                k, g = lax.div(t, 4), h + lax.rem(t, 4)
                r0 = pl.multiple_of(g * ROWS, ROWS)

                @pl.when(jnp.logical_and(k != p, k != mirror))
                def _():
                    landed(zz.at[1, k, rows_of(g)], rb.at[k, g])
                    pl.when(g == 0)(lambda: landed(mm.at[1, k], rmb.at[k]))
                mask_b = mm[1, k, pl.ds(r0, ROWS), :].astype(F32)
                project(lambda r: zz[1, k, r0 + r], mask_b, w_ref, b_ref, 256, stage, bb_ref, group_row(k, g))

        r0 = pl.multiple_of(h * ROWS, ROWS)

        @pl.loop(0, 4)
        def _(k):
            @pl.when(jnp.logical_and(off_diag, k != p))
            def _():
                landed(zz.at[0, k, rows_of(h)], ra.at[k, h])
                pl.when(h == 0)(lambda: landed(mm.at[0, k], rma.at[k]))

            @pl.when(jnp.logical_and(off_diag, k == p))
            def _():
                landed(zz.at[0, k, rows_of(h)], lc.at[h])
            mask_a = mm[asel, k, pl.ds(r0, ROWS), :].astype(F32)
            project(lambda r: zz[asel, k, r0 + r], mask_a, w_ref, b_ref, 0, stage, a_ref, group_row(k, h))

        for at, first, last_row in ((3, 0, 256), (6, 0, 192), (7, 192, 256)):
            @pl.when(h == at)
            def _():
                @pl.loop(0, 128 // 8)
                def _(n):
                    for u in range(8):
                        c = n * 8 + u
                        x_ref[c] += lax.dot_general(a_ref[c, first:last_row, :], bb_ref[c, first:last_row, :], (((0,), (0,)), ((), ())), preferred_element_type=F32)

    third = 3 - 3 * lax.div(q, 2)
    second = q + 1 - 2 * lax.rem(q, 2)
    last = p == third
    slot = jnp.where(p == second, 3, 2)

    @pl.loop(1, 4)
    def _(s):
        m = near_order(q, s, 1)
        lag = jnp.where(last, 2, 0)
        when = jnp.where(last, 3, slot)

        @pl.loop(0, chunks + 2 * lax.div(s, 3))
        def _(h):
            @pl.when(h < chunks)
            def _():
                pass_on(s, m, h)

            @pl.when(jnp.logical_and(s == when, jnp.logical_and(h >= lag, h < chunks + lag)))
            def _():
                compute(h - lag)

    load = pltpu.make_async_copy(keep, a_ref.at[:, 0:128, :], io.at[0])
    load.start()
    load.wait()

    def store(n):
        rows = rows_of(n)
        return pltpu.make_async_copy(bb_ref.at[rows, 0:128, :], out_ref.at[rows], io.at[1])

    @pl.loop(0, chunks)
    def _(n):
        def emit(i, value):
            bb_ref[i, 0:128, :] = jnp.transpose(value.astype(BF16))
        finish_rows(n, x_ref, lambda i: a_ref[i, 0:128, :], lambda i: zz[1, p, i], w_ref, b_ref, wo_ref, bo_ref, lo_ref, stage, emit)
        pl.when(n > 0)(lambda: store(n - 1).start())

    store(jnp.int32(chunks - 1)).start()

    for m in range(4):
        def drain(kind, when):
            @pl.when(when)
            def _():
                landed(col.at[m], ss.at[kind, m])
                landed(mc.at[m], sm.at[kind, m])
        drain(TO_RIGHT, jnp.logical_and(q < 3, m <= q))
        drain(TO_LEFT, jnp.logical_and(q > 0, m >= q))
        drain(2, jnp.logical_and(m != q, m != p))
    for kind in range(3):
        landed(zz.at[1, 0], sp.at[kind])
        landed(mm.at[1, 0], spm.at[kind])
    pltpu.make_async_copy(bb_ref.at[:, 0:128, :], out_ref, io.at[1]).wait()


VM = pl.BlockSpec(memory_space=pltpu.VMEM)
ANY = pl.BlockSpec(memory_space=pl.ANY)
DMA = pltpu.SemaphoreType.DMA


def both_updates(*args):
    n = 128 // ROWS
    block = jax.ShapeDtypeStruct((128, 128, 128), BF16)
    return pl.pallas_call(
        kernel,
        out_shape=[block, jax.ShapeDtypeStruct((4, 128, 128, 128), BF16), block],
        in_specs=[ANY] + [VM] * 7,
        out_specs=[ANY, ANY, ANY],
        scratch_shapes=[
            pltpu.VMEM((2, 640, 128), BF16),
            pltpu.VMEM((2, 640, 128), F32),
            pltpu.VMEM((2, 2, 128, 128), F32),
            pltpu.VMEM((2, 128, 128), BF16),
            pltpu.VMEM((2, 128, 128), F32),
            pltpu.VMEM((2, 2, 128, 128), F32),
            pltpu.VMEM((2, 4, 128, 128, 128), BF16),
            pltpu.VMEM((2, 4, 128, 128), BF16),
            pltpu.VMEM((2, 4, 128, 128), BF16),
            pltpu.VMEM((4, 128, 128), BF16),
            pltpu.VMEM((128, 256, 128), BF16),
            pltpu.VMEM((128, 256, 128), BF16),
            pltpu.VMEM((128, 128, 128), F32),
            pltpu.VMEM((ROWS, 128, 128), F32),
            DMA((4, n)), DMA((4, n)), DMA((4,)), DMA((4,)), DMA((4, 4)), DMA((4, 4)),
            DMA((4, n)), DMA((4, n)), DMA((4, n)), DMA((n,)), DMA((4,)), DMA((4,)), DMA((4,)), DMA((2,)),
            DMA((3, 4)), DMA((3, 4)), DMA((3,)), DMA((3,)),
            pltpu.SemaphoreType.REGULAR((2,)),
        ],
        compiler_params=pltpu.CompilerParams(collective_id=0, has_side_effects=True, vmem_limit_bytes=67043328),
        name='both_updates',
    )(*args)[0]


def solution(mesh):
    pair_spec = P(('batch', 'px'), 'py', None)
    mask_spec = P(('batch', 'px'), 'py')
    whole = P()

    return jax.shard_map(both_updates, mesh=mesh, in_specs=(pair_spec, mask_spec, whole, whole, whole, whole, whole, whole), out_specs=pair_spec, check_vma=False)
```

```python
import functools

import jax
import jax.numpy as jnp
from jax import lax
from jax.experimental import pallas as pl
from jax.experimental.pallas import tpu as pltpu
from jax.sharding import PartitionSpec as P

LN_EPS = 1e-5
MESH = pl.DeviceIdType.MESH
F32, BF16 = jnp.float32, jnp.bfloat16
ROWS, HALF = 16, 8
TO_RIGHT, TO_LEFT, TO_PARTNER, TO_MIRROR = 0, 1, 2, 3


def norm_major(values, gain, shift):
    average = jnp.mean(values, axis=0, keepdims=True)
    centered = values - average
    variance = jnp.mean(centered * centered, axis=0, keepdims=True)
    return centered * lax.rsqrt(variance + LN_EPS) * gain + shift


def remote(src, dst, send_sem, recv_sem, device):
    return pltpu.make_async_remote_copy(src_ref=src, dst_ref=dst, send_sem=send_sem, recv_sem=recv_sem, device_id=device, device_id_type=MESH)


def landed(ref, sem):
    pltpu.make_async_copy(ref, ref, sem).wait()


def project(rows, mask, w_ref, b_ref, base, stage, dst, at):
    w = w_ref[base:base + 256, :]
    for r in range(0, ROWS, 2):
        pair = jnp.concatenate([rows(r), rows(r + 1)], axis=1)
        prod = jnp.dot(w, pair, preferred_element_type=F32)
        for t in range(2):
            gate = prod[:128, 128 * t:128 * t + 128] + b_ref[base:base + 128, :]
            value = prod[128:, 128 * t:128 * t + 128] + b_ref[base + 128:base + 256, :]
            stage[r + t] = mask[r + t:r + t + 1] * jax.nn.sigmoid(gate) * value
    dst[:, pl.ds(at, ROWS), :] = jnp.transpose(stage[...], (1, 0, 2)).astype(BF16)


def finish_rows(n, x_ref, z_row, zn_row, w_ref, b_ref, wo_ref, bo_ref, lo_ref, stage, emit):
    i0 = pl.multiple_of(n * ROWS, ROWS)
    for r in range(0, ROWS, 8):
        x = x_ref[:, pl.ds(i0 + r, 8), :]
        average = jnp.mean(x, axis=0)
        centered = x - average[None]
        variance = jnp.mean(centered * centered, axis=0)
        scale = lax.rsqrt(variance + LN_EPS)
        stage[r:r + 8] = jnp.transpose(centered * scale[None], (1, 0, 2))
    for r in range(0, ROWS, 2):
        pair = [(stage[r + t] * lo_ref[0] + lo_ref[1]).astype(BF16) for t in range(2)]
        update = jnp.dot(wo_ref[...], jnp.concatenate(pair, axis=1), preferred_element_type=F32)
        zn = jnp.concatenate([zn_row(i0 + r), zn_row(i0 + r + 1)], axis=1)
        gate = jnp.dot(w_ref[512:640, :], zn, preferred_element_type=F32)
        for t in range(2):
            lanes = slice(128 * t, 128 * t + 128)
            g = jax.nn.sigmoid(gate[:, lanes] + b_ref[512:640, :])
            emit(i0 + r + t, z_row(i0 + r + t).astype(F32) + g * (update[:, lanes] + bo_ref[...]))


def near_order(q, s, update):
    if update == 0:
        first, second = q + 1 - 2 * lax.rem(q, 2), 2 - lax.div(q, 2)
    else:
        first, second = 2 - lax.div(q, 2), q + 1 - 2 * lax.rem(q, 2)
    third = 3 - 3 * lax.div(q, 2)
    is0, is1, is2, is3 = (jnp.int32(1) * (s == v) for v in range(4))
    return is0 * q + is1 * first + is2 * second + is3 * third


def greet(p, q, everyone):
    barrier = pltpu.get_barrier_semaphore()
    peers = [lax.rem(p + d, 4) for d in (1, 2, 3)] if everyone else [p + 1 - 2 * lax.rem(p, 2), lax.rem(p + 2, 4)]
    for peer in peers:
        pl.semaphore_signal(barrier, inc=1, device_id={'px': peer}, device_id_type=MESH)

    @pl.when(q < 3)
    def _():
        pl.semaphore_signal(barrier, inc=1, device_id={'py': q + 1}, device_id_type=MESH)

    @pl.when(q > 0)
    def _():
        pl.semaphore_signal(barrier, inc=1, device_id={'py': q - 1}, device_id_type=MESH)

    edge = jnp.int32(1) * (q == 0) + jnp.int32(1) * (q == 3)
    return lambda: pl.semaphore_wait(barrier, len(peers) + 2 - edge)


def kernel(z_ref, mask_ref, li_in, w_in, b_in, lo_in, wo_in, bo_in, out_ref, col, keep,
           w_refs, b_refs, li_refs, wo_refs, bo_refs, lo_refs, zz, mb, mm, mc, a_ref, bb_ref, x_ref, stage,
           ra1, rb1, rma1, rmb1, ss1, sm1, rc, ra, rb, lc, rmc, rma, rmb, io, ss, sm, sp, spm, free):
    chunks = 128 // ROWS
    p, q = lax.axis_index('px'), lax.axis_index('py')
    partner, mirror = p + 1 - 2 * lax.rem(p, 2), lax.rem(p + 2, 4)
    right, left = {'py': q + 1}, {'py': q - 1}
    diag = p == q
    off_diag = jnp.logical_not(diag)
    relay = p == lax.rem(q + 2, 4)
    asel = jnp.int32(1) * diag
    bsel = 1 - asel
    plane_peers = [lax.rem(p + d, 4) for d in (1, 2, 3)]

    met = greet(p, q, True)
    load_first = pltpu.make_async_copy(z_ref.at[0:ROWS], bb_ref.at[0:ROWS, 128:256, :], io.at[0])
    load_rest = pltpu.make_async_copy(z_ref.at[ROWS:128], bb_ref.at[ROWS:128, 128:256, :], io.at[1])
    load_first.start()
    load_rest.start()

    def rows_of(h):
        return pl.ds(pl.multiple_of(h * ROWS, ROWS), ROWS)

    w_ref, b_ref, li_ref, wo_ref, bo_ref, lo_ref = (r.at[0] for r in (w_refs, b_refs, li_refs, wo_refs, bo_refs, lo_refs))
    zb = zz

    def along(k, h, kind, dev):
        part = zb.at[0, k, rows_of(h)]
        remote(part, part, ss1.at[kind, k], ra1.at[k, h], dev).start()

    def across(which, k, h, kind, dev):
        remote(zb.at[which, k, rows_of(h)], zb.at[1, k, rows_of(h)], ss1.at[kind, k], rb1.at[k, h], dev).start()

    def along_mask(k, kind, dev):
        remote(mb.at[0, k], mb.at[0, k], sm1.at[kind, k], rma1.at[k], dev).start()

    def across_mask(which, k, kind, dev):
        remote(mb.at[which, k], mb.at[1, k], sm1.at[kind, k], rmb1.at[k], dev).start()

    def spread(k, h, first):
        @pl.when(jnp.logical_and(q < 3, k <= q))
        def _():
            along(k, h, TO_RIGHT, right)
            if first is not None:
                pl.when(first)(lambda: along_mask(k, TO_RIGHT, right))

        @pl.when(jnp.logical_and(q > 0, k >= q))
        def _():
            along(k, h, TO_LEFT, left)
            if first is not None:
                pl.when(first)(lambda: along_mask(k, TO_LEFT, left))

        @pl.when(diag)
        def _():
            across(0, k, h, TO_MIRROR, {'px': mirror})
            across(0, k, h, TO_PARTNER, {'px': partner})
            if first is not None:
                @pl.when(first)
                def _():
                    across_mask(0, k, TO_MIRROR, {'px': mirror})
                    across_mask(0, k, TO_PARTNER, {'px': partner})

    mask = mask_ref[...].astype(F32).astype(BF16)
    mb[0, q] = mask
    mm[1, p] = mask

    def wide(row):
        return jnp.transpose(jnp.broadcast_to(row.astype(F32), (128, 128)))

    for u in range(2):
        ln_rows = li_in[u].astype(F32)
        for t in range(2):
            li_refs[u, t] = wide(ln_rows[t:t + 1])
    def prepare(h):
        for r in range(ROWS):
            i = h * ROWS + r
            zt = jnp.transpose(bb_ref[i, 128:256, :].astype(F32))
            a_ref[i, 128:256, :] = zt.astype(BF16)
            zb[0, q, i] = norm_major(zt, li_ref[0], li_ref[1]).astype(BF16)

    load_first.wait()
    prepare(0)
    met()
    load_rest.wait()

    @pl.loop(1, chunks)
    def _(h):
        prepare(h)
        spread(q, h - 1, h == 1)

    @pl.loop(0, 128)
    def _(c):
        x_ref[c] = jnp.zeros((128, 128), F32)

    spread(q, jnp.int32(chunks - 1), None)

    b_rows, bo_rows = b_in[...].astype(F32), bo_in[...].astype(F32)
    for u in range(2):
        lo_rows = lo_in[u].astype(F32)
        for t in range(2):
            lo_refs[u, t] = wide(lo_rows[t:t + 1])
        bo_refs[u] = wide(bo_rows[u:u + 1])
        wo_refs[u] = jnp.transpose(wo_in[u].astype(F32)).astype(BF16)
        for e in range(0, 640, 128):
            b_refs[u, e:e + 128, :] = wide(b_rows[u:u + 1, e:e + 128])
            w_refs[u, e:e + 128, :] = jnp.transpose(w_in[u, :, e:e + 128].astype(F32)).astype(BF16)

    @pl.loop(0, 4)
    def _(s):
        k = near_order(q, s, 0)

        @pl.loop(0, chunks)
        def _(h):
            @pl.when(s > 0)
            def _():
                landed(zb.at[0, k, rows_of(h)], ra1.at[k, h])
                pl.when(h == 0)(lambda: landed(mb.at[0, k], rma1.at[k]))
                spread(k, h, h == 0)

            @pl.when(jnp.logical_not(diag))
            def _():
                landed(zb.at[1, k, rows_of(h)], rb1.at[k, h])
                pl.when(h == 0)(lambda: landed(mb.at[1, k], rmb1.at[k]))

                @pl.when(relay)
                def _():
                    across(1, k, h, TO_PARTNER, {'px': partner})
                    pl.when(h == 0)(lambda: across_mask(1, k, TO_PARTNER, {'px': partner}))

            r0 = pl.multiple_of(h * ROWS, ROWS)
            mask_a = mb[0, k, pl.ds(r0, ROWS), :].astype(F32)
            project(lambda r: zb[0, k, r0 + r], mask_a, w_ref, b_ref, 0, stage, a_ref, r0)
            mask_b = mb[bsel, k, pl.ds(r0, ROWS), :].astype(F32)
            project(lambda r: zb[bsel, k, r0 + r], mask_b, w_ref, b_ref, 256, stage, bb_ref, r0)

        @pl.loop(0, 128 // 16)
        def _(n):
            for u in range(16):
                c = n * 16 + u
                x_ref[c] += lax.dot_general(a_ref[c, 0:128, :], bb_ref[c, 0:128, :], (((1,), (1,)), ((), ())), preferred_element_type=F32)

    def half_rows(t):
        return pl.ds(pl.multiple_of(t * HALF, HALF), HALF)

    def to_line(src, m, t, kind, dev):
        remote(src, col.at[m, half_rows(t)], ss.at[kind, m], rc.at[m, t], dev).start()

    def to_line_mask(src, m, kind, dev):
        remote(src, mc.at[m], sm.at[kind, m], rmc.at[m], dev).start()

    def plane(src, which, k, h, sem, rsem, dev):
        remote(src, zz.at[which, k, rows_of(h)], sem, rsem, dev).start()

    def own_line(h, first):
        part = zz.at[1, p, rows_of(h)]

        @pl.when(jnp.logical_and(q < 3, q != 2))
        def _():
            for t in (2 * h, 2 * h + 1):
                to_line(zz.at[1, p, half_rows(t)], q, t, TO_RIGHT, right)
            pl.when(first)(lambda: to_line_mask(mm.at[1, p], q, TO_RIGHT, right))

        @pl.when(jnp.logical_and(q > 0, q != 1))
        def _():
            for t in (2 * h, 2 * h + 1):
                to_line(zz.at[1, p, half_rows(t)], q, t, TO_LEFT, left)
            pl.when(first)(lambda: to_line_mask(mm.at[1, p], q, TO_LEFT, left))

        @pl.when(first)
        def _():
            pl.semaphore_wait(free.at[0], 3)
            remote(mm.at[1, p], mm.at[1, p], spm.at[0], rmb.at[p], {'px': mirror}).start()
            remote(mm.at[1, p], mm.at[1, p], spm.at[1], rmb.at[p], {'px': partner}).start()
        plane(part, 1, p, h, sp.at[0], rb.at[p, h], {'px': mirror})
        plane(part, 1, p, h, sp.at[1], rb.at[p, h], {'px': partner})

    @pl.when(relay)
    def _():
        for k in range(4):
            landed(zz.at[1, k], ss1.at[TO_PARTNER, k])
            landed(mb.at[1, k], sm1.at[TO_PARTNER, k])
    for peer in plane_peers:
        pl.semaphore_signal(free.at[0], inc=1, device_id={'px': peer}, device_id_type=MESH)

    @pl.loop(0, chunks)
    def _(n):
        def emit(i, value):
            z1 = value.astype(BF16)
            a_ref[i, 128:256, :] = z1
            zz[1, p, i] = norm_major(z1.astype(F32), li_refs[1, 0], li_refs[1, 1]).astype(BF16)
        finish_rows(n, x_ref, lambda i: a_ref[i, 128:256, :], lambda i: zz[0, q, i], w_ref, b_ref, wo_ref, bo_ref, lo_ref, stage, emit)

        @pl.when(n > 0)
        def _():
            own_line(n - 1, n == 1)

    save = pltpu.make_async_copy(a_ref.at[:, 128:256, :], keep, io.at[0])
    save.start()

    w_ref, b_ref, wo_ref, bo_ref, lo_ref = (r.at[1] for r in (w_refs, b_refs, wo_refs, bo_refs, lo_refs))

    @pl.loop(0, 128)
    def _(c):
        x_ref[c] = jnp.zeros((128, 128), F32)

    own_line(jnp.int32(chunks - 1), jnp.bool_(False))
    inner = lax.rem(q, 3) > 0

    @pl.when(inner)
    def _():
        m = near_order(q, jnp.int32(1), 1)
        kind, outer = 2 - q, {'py': 3 * (q - 1)}
        landed(mc.at[m], rmc.at[m])
        to_line_mask(mc.at[m], m, kind, outer)

        @pl.loop(0, 2 * chunks)
        def _(t):
            landed(col.at[m, half_rows(t)], rc.at[m, t])
            to_line(col.at[m, half_rows(t)], m, t, kind, outer)
        to_line_mask(mm.at[1, p], q, kind, outer)

        @pl.loop(0, 2 * chunks)
        def _(t):
            to_line(zz.at[1, p, half_rows(t)], q, t, kind, outer)

    save.wait()
    for k in range(4):
        def drain0(kind, when):
            @pl.when(when)
            def _():
                landed(zz.at[0, k], ss1.at[kind, k])
                landed(mb.at[0, k], sm1.at[kind, k])
        drain0(TO_RIGHT, jnp.logical_and(q < 3, k <= q))
        drain0(TO_LEFT, jnp.logical_and(q > 0, k >= q))
        drain0(TO_MIRROR, diag)
        drain0(TO_PARTNER, diag)
    for peer in plane_peers:
        pl.semaphore_signal(free.at[1], inc=1, device_id={'px': peer}, device_id_type=MESH)
    pl.semaphore_wait(free.at[1], 3)

    def pass_on(s, m, t):
        @pl.when(jnp.logical_or(s > 1, lax.rem(q, 3) == 0))
        def _():
            landed(col.at[m, half_rows(t)], rc.at[m, t])
            pl.when(t == 0)(lambda: landed(mc.at[m], rmc.at[m]))
        part = col.at[m, half_rows(t)]

        @pl.when(jnp.logical_and(s > 1, jnp.logical_and(q < 3, m < q)))
        def _():
            to_line(part, m, t, TO_RIGHT, right)
            pl.when(t == 0)(lambda: to_line_mask(mc.at[m], m, TO_RIGHT, right))

        @pl.when(jnp.logical_and(s > 1, jnp.logical_and(q > 0, m > q)))
        def _():
            to_line(part, m, t, TO_LEFT, left)
            pl.when(t == 0)(lambda: to_line_mask(mc.at[m], m, TO_LEFT, left))

        @pl.when(m != p)
        def _():
            remote(part, zz.at[0, p, half_rows(t)], ss.at[2, m], ra.at[p, t], {'px': m}).start()
            pl.when(t == 0)(lambda: remote(mc.at[m], mm.at[0, p], sm.at[2, m], rma.at[p], {'px': m}).start())

        @pl.when(m == p)
        def _():
            pltpu.make_async_copy(part, zz.at[0, p, half_rows(t)], lc.at[t]).start()

            @pl.when(t == 0)
            def _():
                mm[0, p] = mc[p]

        @pl.when(jnp.logical_and(s == 1, lax.rem(t, 2) == 1))
        def _():
            h = lax.div(t, 2)
            landed(zz.at[1, mirror, rows_of(h)], rb.at[mirror, h])
            plane(zz.at[1, mirror, rows_of(h)], 1, mirror, h, sp.at[2], rb.at[mirror, h], {'px': partner})

            @pl.when(h == 0)
            def _():
                landed(mm.at[1, mirror], rmb.at[mirror])
                remote(mm.at[1, mirror], mm.at[1, mirror], spm.at[2], rmb.at[mirror], {'px': partner}).start()

    def group_row(k, h):
        return pl.multiple_of(lax.rem(h, 4) * 64 + k * ROWS, ROWS)

    def compute(h):
        @pl.when(lax.rem(h, 4) == 0)
        def _():
            @pl.loop(0, 16)
            def _(t):
                k, g = lax.div(t, 4), h + lax.rem(t, 4)
                r0 = pl.multiple_of(g * ROWS, ROWS)

                @pl.when(jnp.logical_and(k != p, k != mirror))
                def _():
                    landed(zz.at[1, k, rows_of(g)], rb.at[k, g])
                    pl.when(g == 0)(lambda: landed(mm.at[1, k], rmb.at[k]))
                mask_b = mm[1, k, pl.ds(r0, ROWS), :].astype(F32)
                project(lambda r: zz[1, k, r0 + r], mask_b, w_ref, b_ref, 256, stage, bb_ref, group_row(k, g))

        r0 = pl.multiple_of(h * ROWS, ROWS)

        @pl.loop(0, 4)
        def _(k):
            @pl.when(jnp.logical_and(off_diag, k != p))
            def _():
                for t in (2 * h, 2 * h + 1):
                    landed(zz.at[0, k, half_rows(t)], ra.at[k, t])
                pl.when(h == 0)(lambda: landed(mm.at[0, k], rma.at[k]))

            @pl.when(jnp.logical_and(off_diag, k == p))
            def _():
                for t in (2 * h, 2 * h + 1):
                    landed(zz.at[0, k, half_rows(t)], lc.at[t])
            mask_a = mm[asel, k, pl.ds(r0, ROWS), :].astype(F32)
            project(lambda r: zz[asel, k, r0 + r], mask_a, w_ref, b_ref, 0, stage, a_ref, group_row(k, h))

        @pl.when(h == 7)
        def _():
            landed(zz.at[1, 0], sp.at[2])
            pltpu.make_async_copy(keep, zz.at[1, mirror], io.at[0]).start()

        for at, first, last_row in ((3, 0, 256), (6, 0, 192), (7, 192, 256)):
            @pl.when(h == at)
            def _():
                @pl.loop(0, 128 // 8)
                def _(n):
                    for u in range(8):
                        c = n * 8 + u
                        x_ref[c] += lax.dot_general(a_ref[c, first:last_row, :], bb_ref[c, first:last_row, :], (((0,), (0,)), ((), ())), preferred_element_type=F32)

    third = 3 - 3 * lax.div(q, 2)
    second = q + 1 - 2 * lax.rem(q, 2)
    last = p == third
    slot = jnp.where(p == second, 3, 2)

    @pl.loop(1, 4)
    def _(s):
        m = near_order(q, s, 1)
        when = jnp.where(last, 3, slot)

        @pl.loop(0, chunks)
        def _(h):
            @pl.loop(0, 2)
            def _(t):
                pass_on(s, m, 2 * h + t)

            @pl.when(s == when)
            def _():
                compute(h)

    pltpu.make_async_copy(keep, zz.at[1, mirror], io.at[0]).wait()

    def store(n):
        rows = rows_of(n)
        return pltpu.make_async_copy(bb_ref.at[rows, 0:128, :], out_ref.at[rows], io.at[1])

    @pl.loop(0, chunks)
    def _(n):
        def emit(i, value):
            bb_ref[i, 0:128, :] = jnp.transpose(value.astype(BF16))
        finish_rows(n, x_ref, lambda i: zz[1, mirror, i], lambda i: zz[1, p, i], w_ref, b_ref, wo_ref, bo_ref, lo_ref, stage, emit)
        pl.when(n > 0)(lambda: store(n - 1).start())

    store(jnp.int32(chunks - 1)).start()

    for m in range(4):
        def drain(kind, when):
            @pl.when(when)
            def _():
                landed(col.at[m], ss.at[kind, m])
                landed(mc.at[m], sm.at[kind, m])
        drain(TO_RIGHT, jnp.logical_and(q < 3, m <= q))
        drain(TO_LEFT, jnp.logical_and(q > 0, m >= q))
        drain(2, jnp.logical_and(m != q, m != p))
    for kind in range(3):
        if kind < 2:
            landed(zz.at[1, 0], sp.at[kind])
        landed(mm.at[1, 0], spm.at[kind])
    pltpu.make_async_copy(bb_ref.at[:, 0:128, :], out_ref, io.at[1]).wait()


VM = pl.BlockSpec(memory_space=pltpu.VMEM)
ANY = pl.BlockSpec(memory_space=pl.ANY)
DMA = pltpu.SemaphoreType.DMA


def both_updates(*args):
    n = 128 // ROWS
    block = jax.ShapeDtypeStruct((128, 128, 128), BF16)
    return pl.pallas_call(
        kernel,
        out_shape=[block, jax.ShapeDtypeStruct((4, 128, 128, 128), BF16), block],
        in_specs=[ANY] + [VM] * 7,
        out_specs=[ANY, ANY, ANY],
        scratch_shapes=[
            pltpu.VMEM((2, 640, 128), BF16),
            pltpu.VMEM((2, 640, 128), F32),
            pltpu.VMEM((2, 2, 128, 128), F32),
            pltpu.VMEM((2, 128, 128), BF16),
            pltpu.VMEM((2, 128, 128), F32),
            pltpu.VMEM((2, 2, 128, 128), F32),
            pltpu.VMEM((2, 4, 128, 128, 128), BF16),
            pltpu.VMEM((2, 4, 128, 128), BF16),
            pltpu.VMEM((2, 4, 128, 128), BF16),
            pltpu.VMEM((4, 128, 128), BF16),
            pltpu.VMEM((128, 256, 128), BF16),
            pltpu.VMEM((128, 256, 128), BF16),
            pltpu.VMEM((128, 128, 128), F32),
            pltpu.VMEM((ROWS, 128, 128), F32),
            DMA((4, n)), DMA((4, n)), DMA((4,)), DMA((4,)), DMA((4, 4)), DMA((4, 4)),
            DMA((4, 2 * n)), DMA((4, 2 * n)), DMA((4, n)), DMA((2 * n,)), DMA((4,)), DMA((4,)), DMA((4,)), DMA((2,)),
            DMA((3, 4)), DMA((3, 4)), DMA((3,)), DMA((3,)),
            pltpu.SemaphoreType.REGULAR((2,)),
        ],
        compiler_params=pltpu.CompilerParams(collective_id=0, has_side_effects=True, vmem_limit_bytes=67043328),
        name='both_updates',
    )(*args)[0]


def solution(mesh):
    pair_spec = P(('batch', 'px'), 'py', None)
    mask_spec = P(('batch', 'px'), 'py')
    whole = P()

    return jax.shard_map(both_updates, mesh=mesh, in_specs=(pair_spec, mask_spec, whole, whole, whole, whole, whole, whole), out_specs=pair_spec, check_vma=False)
```

```python
import functools

import jax
import jax.numpy as jnp
from jax import lax
from jax.experimental import pallas as pl
from jax.experimental.pallas import tpu as pltpu
from jax.sharding import PartitionSpec as P

LN_EPS = 1e-5
MESH = pl.DeviceIdType.MESH
F32, BF16 = jnp.float32, jnp.bfloat16
ROWS, HALF = 16, 8
TO_RIGHT, TO_LEFT, TO_PARTNER, TO_MIRROR = 0, 1, 2, 3


def norm_major(values, gain, shift):
    average = jnp.mean(values, axis=0, keepdims=True)
    centered = values - average
    variance = jnp.mean(centered * centered, axis=0, keepdims=True)
    return centered * lax.rsqrt(variance + LN_EPS) * gain + shift


def remote(src, dst, send_sem, recv_sem, device):
    return pltpu.make_async_remote_copy(src_ref=src, dst_ref=dst, send_sem=send_sem, recv_sem=recv_sem, device_id=device, device_id_type=MESH)


def landed(ref, sem):
    pltpu.make_async_copy(ref, ref, sem).wait()


def project(rows, mask, w_ref, b_ref, base, stage, dst, at):
    w = w_ref[base:base + 256, :]
    for r in range(0, ROWS, 2):
        pair = jnp.concatenate([rows(r), rows(r + 1)], axis=1)
        prod = jnp.dot(w, pair, preferred_element_type=F32)
        for t in range(2):
            gate = prod[:128, 128 * t:128 * t + 128] + b_ref[base:base + 128, :]
            value = prod[128:, 128 * t:128 * t + 128] + b_ref[base + 128:base + 256, :]
            stage[r + t] = mask[r + t:r + t + 1] * jax.nn.sigmoid(gate) * value
    dst[:, pl.ds(at, ROWS), :] = jnp.transpose(stage[...], (1, 0, 2)).astype(BF16)


def finish_rows(n, x_ref, z_row, zn_row, w_ref, b_ref, wo_ref, bo_ref, lo_ref, stage, emit):
    i0 = pl.multiple_of(n * ROWS, ROWS)
    for r in range(0, ROWS, 8):
        x = x_ref[:, pl.ds(i0 + r, 8), :]
        average = jnp.mean(x, axis=0)
        centered = x - average[None]
        variance = jnp.mean(centered * centered, axis=0)
        scale = lax.rsqrt(variance + LN_EPS)
        stage[r:r + 8] = jnp.transpose(centered * scale[None], (1, 0, 2))
    for r in range(0, ROWS, 2):
        pair = [(stage[r + t] * lo_ref[0] + lo_ref[1]).astype(BF16) for t in range(2)]
        update = jnp.dot(wo_ref[...], jnp.concatenate(pair, axis=1), preferred_element_type=F32)
        zn = jnp.concatenate([zn_row(i0 + r), zn_row(i0 + r + 1)], axis=1)
        gate = jnp.dot(w_ref[512:640, :], zn, preferred_element_type=F32)
        for t in range(2):
            lanes = slice(128 * t, 128 * t + 128)
            g = jax.nn.sigmoid(gate[:, lanes] + b_ref[512:640, :])
            emit(i0 + r + t, z_row(i0 + r + t).astype(F32) + g * (update[:, lanes] + bo_ref[...]))


def near_order(q, s, update):
    if update == 0:
        first, second = q + 1 - 2 * lax.rem(q, 2), 2 - lax.div(q, 2)
    else:
        first, second = 2 - lax.div(q, 2), q + 1 - 2 * lax.rem(q, 2)
    third = 3 - 3 * lax.div(q, 2)
    is0, is1, is2, is3 = (jnp.int32(1) * (s == v) for v in range(4))
    return is0 * q + is1 * first + is2 * second + is3 * third


def greet(p, q, everyone):
    barrier = pltpu.get_barrier_semaphore()
    peers = [lax.rem(p + d, 4) for d in (1, 2, 3)] if everyone else [p + 1 - 2 * lax.rem(p, 2), lax.rem(p + 2, 4)]
    for peer in peers:
        pl.semaphore_signal(barrier, inc=1, device_id={'px': peer}, device_id_type=MESH)

    @pl.when(q < 3)
    def _():
        pl.semaphore_signal(barrier, inc=1, device_id={'py': q + 1}, device_id_type=MESH)

    @pl.when(q > 0)
    def _():
        pl.semaphore_signal(barrier, inc=1, device_id={'py': q - 1}, device_id_type=MESH)

    edge = jnp.int32(1) * (q == 0) + jnp.int32(1) * (q == 3)
    return lambda: pl.semaphore_wait(barrier, len(peers) + 2 - edge)


def kernel(z_ref, mask_ref, li_in, w_in, b_in, lo_in, wo_in, bo_in, out_ref, col, keep,
           w_refs, b_refs, li_refs, wo_refs, bo_refs, lo_refs, zz, mb, mm, mc, a_ref, bb_ref, x_ref, stage,
           ra1, rb1, rma1, rmb1, ss1, sm1, rc, ra, rb, lc, rmc, rma, rmb, io, ss, sm, sp, spm, free):
    chunks = 128 // ROWS
    p, q = lax.axis_index('px'), lax.axis_index('py')
    partner, mirror = p + 1 - 2 * lax.rem(p, 2), lax.rem(p + 2, 4)
    right, left = {'py': q + 1}, {'py': q - 1}
    diag = p == q
    off_diag = jnp.logical_not(diag)
    relay = p == lax.rem(q + 2, 4)
    asel = jnp.int32(1) * diag
    bsel = 1 - asel
    plane_peers = [lax.rem(p + d, 4) for d in (1, 2, 3)]

    met = greet(p, q, True)
    load_first = pltpu.make_async_copy(z_ref.at[0:ROWS], bb_ref.at[0:ROWS, 128:256, :], io.at[0])
    load_rest = pltpu.make_async_copy(z_ref.at[ROWS:128], bb_ref.at[ROWS:128, 128:256, :], io.at[1])
    load_first.start()
    load_rest.start()

    def rows_of(h):
        return pl.ds(pl.multiple_of(h * ROWS, ROWS), ROWS)

    w_ref, b_ref, li_ref, wo_ref, bo_ref, lo_ref = (r.at[0] for r in (w_refs, b_refs, li_refs, wo_refs, bo_refs, lo_refs))
    zb = zz

    def along(k, h, kind, dev):
        part = zb.at[0, k, rows_of(h)]
        remote(part, part, ss1.at[kind, k], ra1.at[k, h], dev).start()

    def across(which, k, h, kind, dev):
        remote(zb.at[which, k, rows_of(h)], zb.at[1, k, rows_of(h)], ss1.at[kind, k], rb1.at[k, h], dev).start()

    def along_mask(k, kind, dev):
        remote(mb.at[0, k], mb.at[0, k], sm1.at[kind, k], rma1.at[k], dev).start()

    def across_mask(which, k, kind, dev):
        remote(mb.at[which, k], mb.at[1, k], sm1.at[kind, k], rmb1.at[k], dev).start()

    def spread(k, h, first):
        @pl.when(jnp.logical_and(q < 3, k <= q))
        def _():
            along(k, h, TO_RIGHT, right)
            if first is not None:
                pl.when(first)(lambda: along_mask(k, TO_RIGHT, right))

        @pl.when(jnp.logical_and(q > 0, k >= q))
        def _():
            along(k, h, TO_LEFT, left)
            if first is not None:
                pl.when(first)(lambda: along_mask(k, TO_LEFT, left))

        @pl.when(diag)
        def _():
            across(0, k, h, TO_MIRROR, {'px': mirror})
            across(0, k, h, TO_PARTNER, {'px': partner})
            if first is not None:
                @pl.when(first)
                def _():
                    across_mask(0, k, TO_MIRROR, {'px': mirror})
                    across_mask(0, k, TO_PARTNER, {'px': partner})

    mask = mask_ref[...].astype(F32).astype(BF16)
    mb[0, q] = mask
    mm[1, p] = mask

    def wide(row):
        return jnp.transpose(jnp.broadcast_to(row.astype(F32), (128, 128)))

    for u in range(2):
        ln_rows = li_in[u].astype(F32)
        for t in range(2):
            li_refs[u, t] = wide(ln_rows[t:t + 1])
    def prepare(h):
        for r in range(ROWS):
            i = h * ROWS + r
            zt = jnp.transpose(bb_ref[i, 128:256, :].astype(F32))
            a_ref[i, 128:256, :] = zt.astype(BF16)
            zb[0, q, i] = norm_major(zt, li_ref[0], li_ref[1]).astype(BF16)

    load_first.wait()
    prepare(0)
    met()
    load_rest.wait()

    @pl.loop(1, chunks)
    def _(h):
        prepare(h)
        spread(q, h - 1, h == 1)

    @pl.loop(0, 128)
    def _(c):
        x_ref[c] = jnp.zeros((128, 128), F32)

    spread(q, jnp.int32(chunks - 1), None)

    b_rows, bo_rows = b_in[...].astype(F32), bo_in[...].astype(F32)
    for u in range(2):
        lo_rows = lo_in[u].astype(F32)
        for t in range(2):
            lo_refs[u, t] = wide(lo_rows[t:t + 1])
        bo_refs[u] = wide(bo_rows[u:u + 1])
        wo_refs[u] = jnp.transpose(wo_in[u].astype(F32)).astype(BF16)
        for e in range(0, 640, 128):
            b_refs[u, e:e + 128, :] = wide(b_rows[u:u + 1, e:e + 128])
            w_refs[u, e:e + 128, :] = jnp.transpose(w_in[u, :, e:e + 128].astype(F32)).astype(BF16)

    @pl.loop(0, 4)
    def _(s):
        k = near_order(q, s, 0)

        @pl.loop(0, chunks)
        def _(h):
            @pl.when(s > 0)
            def _():
                landed(zb.at[0, k, rows_of(h)], ra1.at[k, h])
                pl.when(h == 0)(lambda: landed(mb.at[0, k], rma1.at[k]))
                spread(k, h, h == 0)

            @pl.when(jnp.logical_not(diag))
            def _():
                landed(zb.at[1, k, rows_of(h)], rb1.at[k, h])
                pl.when(h == 0)(lambda: landed(mb.at[1, k], rmb1.at[k]))

                @pl.when(relay)
                def _():
                    across(1, k, h, TO_PARTNER, {'px': partner})
                    pl.when(h == 0)(lambda: across_mask(1, k, TO_PARTNER, {'px': partner}))

            r0 = pl.multiple_of(h * ROWS, ROWS)
            mask_a = mb[0, k, pl.ds(r0, ROWS), :].astype(F32)
            project(lambda r: zb[0, k, r0 + r], mask_a, w_ref, b_ref, 0, stage, a_ref, r0)
            mask_b = mb[bsel, k, pl.ds(r0, ROWS), :].astype(F32)
            project(lambda r: zb[bsel, k, r0 + r], mask_b, w_ref, b_ref, 256, stage, bb_ref, r0)

        @pl.loop(0, 128 // 16)
        def _(n):
            for u in range(16):
                c = n * 16 + u
                x_ref[c] += lax.dot_general(a_ref[c, 0:128, :], bb_ref[c, 0:128, :], (((1,), (1,)), ((), ())), preferred_element_type=F32)

    def half_rows(t):
        return pl.ds(pl.multiple_of(t * HALF, HALF), HALF)

    def to_line(src, m, t, kind, dev):
        remote(src, col.at[m, half_rows(t)], ss.at[kind, m], rc.at[m, t], dev).start()

    def to_line_mask(src, m, kind, dev):
        remote(src, mc.at[m], sm.at[kind, m], rmc.at[m], dev).start()

    def plane(src, which, k, h, sem, rsem, dev):
        remote(src, zz.at[which, k, rows_of(h)], sem, rsem, dev).start()

    def own_line(h, first):
        part = zz.at[1, p, rows_of(h)]

        @pl.when(jnp.logical_and(q < 3, q != 2))
        def _():
            for t in (2 * h, 2 * h + 1):
                to_line(zz.at[1, p, half_rows(t)], q, t, TO_RIGHT, right)
            pl.when(first)(lambda: to_line_mask(mm.at[1, p], q, TO_RIGHT, right))

        @pl.when(jnp.logical_and(q > 0, q != 1))
        def _():
            for t in (2 * h, 2 * h + 1):
                to_line(zz.at[1, p, half_rows(t)], q, t, TO_LEFT, left)
            pl.when(first)(lambda: to_line_mask(mm.at[1, p], q, TO_LEFT, left))

        @pl.when(first)
        def _():
            pl.semaphore_wait(free.at[0], 3)
            remote(mm.at[1, p], mm.at[1, p], spm.at[0], rmb.at[p], {'px': mirror}).start()
            remote(mm.at[1, p], mm.at[1, p], spm.at[1], rmb.at[p], {'px': partner}).start()
        plane(part, 1, p, h, sp.at[0], rb.at[p, h], {'px': mirror})
        plane(part, 1, p, h, sp.at[1], rb.at[p, h], {'px': partner})

    @pl.when(relay)
    def _():
        for k in range(4):
            landed(zz.at[1, k], ss1.at[TO_PARTNER, k])
            landed(mb.at[1, k], sm1.at[TO_PARTNER, k])
    for peer in plane_peers:
        pl.semaphore_signal(free.at[0], inc=1, device_id={'px': peer}, device_id_type=MESH)

    @pl.loop(0, chunks)
    def _(n):
        def emit(i, value):
            z1 = value.astype(BF16)
            a_ref[i, 128:256, :] = z1
            zz[1, p, i] = norm_major(z1.astype(F32), li_refs[1, 0], li_refs[1, 1]).astype(BF16)
        finish_rows(n, x_ref, lambda i: a_ref[i, 128:256, :], lambda i: zz[0, q, i], w_ref, b_ref, wo_ref, bo_ref, lo_ref, stage, emit)

        @pl.when(n > 0)
        def _():
            own_line(n - 1, n == 1)

    save = pltpu.make_async_copy(a_ref.at[:, 128:256, :], keep, io.at[0])
    save.start()

    w_ref, b_ref, wo_ref, bo_ref, lo_ref = (r.at[1] for r in (w_refs, b_refs, wo_refs, bo_refs, lo_refs))

    @pl.loop(0, 128)
    def _(c):
        x_ref[c] = jnp.zeros((128, 128), F32)

    own_line(jnp.int32(chunks - 1), jnp.bool_(False))
    inner = lax.rem(q, 3) > 0

    @pl.when(inner)
    def _():
        m = near_order(q, jnp.int32(1), 1)
        kind, outer = 2 - q, {'py': 3 * (q - 1)}
        landed(mc.at[m], rmc.at[m])
        to_line_mask(mc.at[m], m, kind, outer)

        @pl.loop(0, 2 * chunks)
        def _(t):
            landed(col.at[m, half_rows(t)], rc.at[m, t])
            to_line(col.at[m, half_rows(t)], m, t, kind, outer)
        to_line_mask(mm.at[1, p], q, kind, outer)

        @pl.loop(0, 2 * chunks)
        def _(t):
            to_line(zz.at[1, p, half_rows(t)], q, t, kind, outer)

    save.wait()
    for k in range(4):
        def drain0(kind, when):
            @pl.when(when)
            def _():
                landed(zz.at[0, k], ss1.at[kind, k])
                landed(mb.at[0, k], sm1.at[kind, k])
        drain0(TO_RIGHT, jnp.logical_and(q < 3, k <= q))
        drain0(TO_LEFT, jnp.logical_and(q > 0, k >= q))
        drain0(TO_MIRROR, diag)
        drain0(TO_PARTNER, diag)
    for peer in plane_peers:
        pl.semaphore_signal(free.at[1], inc=1, device_id={'px': peer}, device_id_type=MESH)
    pl.semaphore_wait(free.at[1], 3)

    def pass_on(s, m, t):
        @pl.when(jnp.logical_or(s > 1, lax.rem(q, 3) == 0))
        def _():
            landed(col.at[m, half_rows(t)], rc.at[m, t])
            pl.when(t == 0)(lambda: landed(mc.at[m], rmc.at[m]))
        part = col.at[m, half_rows(t)]

        @pl.when(jnp.logical_and(s > 1, jnp.logical_and(q < 3, m < q)))
        def _():
            to_line(part, m, t, TO_RIGHT, right)
            pl.when(t == 0)(lambda: to_line_mask(mc.at[m], m, TO_RIGHT, right))

        @pl.when(jnp.logical_and(s > 1, jnp.logical_and(q > 0, m > q)))
        def _():
            to_line(part, m, t, TO_LEFT, left)
            pl.when(t == 0)(lambda: to_line_mask(mc.at[m], m, TO_LEFT, left))

        @pl.when(m != p)
        def _():
            remote(part, zz.at[0, p, half_rows(t)], ss.at[2, m], ra.at[p, t], {'px': m}).start()
            pl.when(t == 0)(lambda: remote(mc.at[m], mm.at[0, p], sm.at[2, m], rma.at[p], {'px': m}).start())

        @pl.when(m == p)
        def _():
            pltpu.make_async_copy(part, zz.at[0, p, half_rows(t)], lc.at[t]).start()

            @pl.when(t == 0)
            def _():
                mm[0, p] = mc[p]

        @pl.when(jnp.logical_and(s == 1, lax.rem(t, 2) == 1))
        def _():
            h = lax.div(t, 2)
            landed(zz.at[1, mirror, rows_of(h)], rb.at[mirror, h])
            plane(zz.at[1, mirror, rows_of(h)], 1, mirror, h, sp.at[2], rb.at[mirror, h], {'px': partner})

            @pl.when(h == 0)
            def _():
                landed(mm.at[1, mirror], rmb.at[mirror])
                remote(mm.at[1, mirror], mm.at[1, mirror], spm.at[2], rmb.at[mirror], {'px': partner}).start()

    def group_row(k, h):
        return pl.multiple_of(lax.rem(h, 4) * 64 + k * ROWS, ROWS)

    def compute(h):
        @pl.when(lax.rem(h, 4) == 0)
        def _():
            @pl.loop(0, 16)
            def _(t):
                k, g = lax.div(t, 4), h + lax.rem(t, 4)
                r0 = pl.multiple_of(g * ROWS, ROWS)

                @pl.when(jnp.logical_and(k != p, k != mirror))
                def _():
                    landed(zz.at[1, k, rows_of(g)], rb.at[k, g])
                    pl.when(g == 0)(lambda: landed(mm.at[1, k], rmb.at[k]))
                mask_b = mm[1, k, pl.ds(r0, ROWS), :].astype(F32)
                project(lambda r: zz[1, k, r0 + r], mask_b, w_ref, b_ref, 256, stage, bb_ref, group_row(k, g))

        r0 = pl.multiple_of(h * ROWS, ROWS)

        @pl.loop(0, 4)
        def _(k):
            @pl.when(jnp.logical_and(off_diag, k != p))
            def _():
                for t in (2 * h, 2 * h + 1):
                    landed(zz.at[0, k, half_rows(t)], ra.at[k, t])
                pl.when(h == 0)(lambda: landed(mm.at[0, k], rma.at[k]))

            @pl.when(jnp.logical_and(off_diag, k == p))
            def _():
                for t in (2 * h, 2 * h + 1):
                    landed(zz.at[0, k, half_rows(t)], lc.at[t])
            mask_a = mm[asel, k, pl.ds(r0, ROWS), :].astype(F32)
            project(lambda r: zz[asel, k, r0 + r], mask_a, w_ref, b_ref, 0, stage, a_ref, group_row(k, h))

        @pl.when(h == 7)
        def _():
            landed(zz.at[1, 0], sp.at[2])
            pltpu.make_async_copy(keep, zz.at[1, mirror], io.at[0]).start()

        for at, first, last_row in ((3, 0, 256), (6, 0, 192), (7, 192, 256)):
            @pl.when(h == at)
            def _():
                @pl.loop(0, 128 // 16)
                def _(n):
                    for u in range(16):
                        c = n * 16 + u
                        x_ref[c] += lax.dot_general(a_ref[c, first:last_row, :], bb_ref[c, first:last_row, :], (((0,), (0,)), ((), ())), preferred_element_type=F32)

    third = 3 - 3 * lax.div(q, 2)
    second = q + 1 - 2 * lax.rem(q, 2)
    last = p == third
    slot = jnp.where(p == second, 3, 2)

    @pl.loop(1, 4)
    def _(s):
        m = near_order(q, s, 1)
        when = jnp.where(last, 3, slot)

        @pl.loop(0, chunks)
        def _(h):
            @pl.loop(0, 2)
            def _(t):
                pass_on(s, m, 2 * h + t)

            @pl.when(s == when)
            def _():
                compute(h)

    pltpu.make_async_copy(keep, zz.at[1, mirror], io.at[0]).wait()

    def store(n):
        rows = rows_of(n)
        return pltpu.make_async_copy(bb_ref.at[rows, 0:128, :], out_ref.at[rows], io.at[1])

    @pl.loop(0, chunks)
    def _(n):
        def emit(i, value):
            bb_ref[i, 0:128, :] = jnp.transpose(value.astype(BF16))
        finish_rows(n, x_ref, lambda i: zz[1, mirror, i], lambda i: zz[1, p, i], w_ref, b_ref, wo_ref, bo_ref, lo_ref, stage, emit)
        pl.when(n > 0)(lambda: store(n - 1).start())

    store(jnp.int32(chunks - 1)).start()

    for m in range(4):
        def drain(kind, when):
            @pl.when(when)
            def _():
                landed(col.at[m], ss.at[kind, m])
                landed(mc.at[m], sm.at[kind, m])
        drain(TO_RIGHT, jnp.logical_and(q < 3, m <= q))
        drain(TO_LEFT, jnp.logical_and(q > 0, m >= q))
        drain(2, jnp.logical_and(m != q, m != p))
    for kind in range(3):
        if kind < 2:
            landed(zz.at[1, 0], sp.at[kind])
        landed(mm.at[1, 0], spm.at[kind])
    pltpu.make_async_copy(bb_ref.at[:, 0:128, :], out_ref, io.at[1]).wait()


VM = pl.BlockSpec(memory_space=pltpu.VMEM)
ANY = pl.BlockSpec(memory_space=pl.ANY)
DMA = pltpu.SemaphoreType.DMA


def both_updates(*args):
    n = 128 // ROWS
    block = jax.ShapeDtypeStruct((128, 128, 128), BF16)
    return pl.pallas_call(
        kernel,
        out_shape=[block, jax.ShapeDtypeStruct((4, 128, 128, 128), BF16), block],
        in_specs=[ANY] + [VM] * 7,
        out_specs=[ANY, ANY, ANY],
        scratch_shapes=[
            pltpu.VMEM((2, 640, 128), BF16),
            pltpu.VMEM((2, 640, 128), F32),
            pltpu.VMEM((2, 2, 128, 128), F32),
            pltpu.VMEM((2, 128, 128), BF16),
            pltpu.VMEM((2, 128, 128), F32),
            pltpu.VMEM((2, 2, 128, 128), F32),
            pltpu.VMEM((2, 4, 128, 128, 128), BF16),
            pltpu.VMEM((2, 4, 128, 128), BF16),
            pltpu.VMEM((2, 4, 128, 128), BF16),
            pltpu.VMEM((4, 128, 128), BF16),
            pltpu.VMEM((128, 256, 128), BF16),
            pltpu.VMEM((128, 256, 128), BF16),
            pltpu.VMEM((128, 128, 128), F32),
            pltpu.VMEM((ROWS, 128, 128), F32),
            DMA((4, n)), DMA((4, n)), DMA((4,)), DMA((4,)), DMA((4, 4)), DMA((4, 4)),
            DMA((4, 2 * n)), DMA((4, 2 * n)), DMA((4, n)), DMA((2 * n,)), DMA((4,)), DMA((4,)), DMA((4,)), DMA((2,)),
            DMA((3, 4)), DMA((3, 4)), DMA((3,)), DMA((3,)),
            pltpu.SemaphoreType.REGULAR((2,)),
        ],
        compiler_params=pltpu.CompilerParams(collective_id=0, has_side_effects=True, vmem_limit_bytes=67043328),
        name='both_updates',
    )(*args)[0]


def solution(mesh):
    pair_spec = P(('batch', 'px'), 'py', None)
    mask_spec = P(('batch', 'px'), 'py')
    whole = P()

    return jax.shard_map(both_updates, mesh=mesh, in_specs=(pair_spec, mask_spec, whole, whole, whole, whole, whole, whole), out_specs=pair_spec, check_vma=False)
```
